128 devices in a mesh: grp: 16 (over z, x), blk: 8 (over y, core).
Axes of the slice: x: 4, y: 4, z: 4, core: 2. Of those that a mesh axis runs over, the one named last changes fastest.
Arguments:
- embeddings: bfloat16 [65536, 1024], P(('grp', 'blk')), may hold values from -60 to 60
- cluster_ids: int32 [65536], P(('grp', 'blk')), may hold values from 0 to 15, as said below
- rank_key: int32 [65536], P(('grp', 'blk')), may hold values from 0 to 65535, each once
Outputs:
- best: float32 [65536], P(('grp', 'blk'))
The draws below stay inside these ranges and needn't reach their ends.
Inputs may be any that keep to these rules, and one draw needn't show every extreme that they name: `cluster_ids`: on every device, at most 64 of its rows have cluster ids congruent to one value modulo 16, and for some value exactly that many.
All inputs are finite; a program needn't handle non-finite values.
Results may differ from the reference program's by a relative error of at most 0.0005.
Values may be sent and summed in bfloat16 or wider, within the bound.
A program may use at most 64 MiB of HBM per device.

```python
import math
import jax
import jax.numpy as jnp
from jax import lax

D = 1024
ROWS_DEV = 512
CL_GRP = 1
ROWS = 65536
N_GRP = 16
N_BLK = 8


def cluster_layout(key):
    devices = N_GRP * N_BLK
    room = 2 * ROWS_DEV // N_GRP
    k_hot, k_pick, k_slot, k_within = jax.random.split(jax.random.fold_in(key, 11), 4)
    hot = jax.random.permutation(k_hot, N_GRP)[:2]
    full_group = hot[jax.random.randint(k_pick, (devices,), 0, 2)]

    def device_rows(dkey, favoured):
        k_first, k_second = jax.random.split(dkey)
        shuffled = jax.random.permutation(k_first, 2 * ROWS_DEV).astype(jnp.int32)
        owner_of = shuffled // room
        score = jnp.where(owner_of == favoured, 0, 1) * (2 * ROWS_DEV) + jnp.arange(2 * ROWS_DEV, dtype=jnp.int32)
        picked = shuffled[jnp.argsort(score)[:ROWS_DEV]]
        mixed = jax.random.permutation(k_second, picked)
        return mixed // room
    owners = jax.vmap(device_rows)(jax.random.split(k_slot, devices), full_group).reshape(-1)
    within = jnp.min(jax.random.randint(k_within, (3, ROWS_DEV * devices), 0, CL_GRP), axis=0)
    return (owners + N_GRP * within).astype(jnp.int32)


def pair_layout(key, clusters):
    total = clusters.shape[0]
    k_order, k_flag = jax.random.split(jax.random.fold_in(key, 37))
    shuffled = jax.random.permutation(k_order, total).astype(jnp.int32)
    sort_key = clusters * total + shuffled
    order = jnp.argsort(sort_key).astype(jnp.int32)
    position = jnp.zeros((total,), jnp.int32).at[order].set(jnp.arange(total, dtype=jnp.int32))
    mate = order[jnp.bitwise_xor(position, 1)]
    leader = order[position // 2 * 2]
    flags = jax.random.randint(k_flag, (total // 2,), 0, 2)
    paired = (clusters[mate] == clusters) & (flags[position // 2] == 1)
    return (paired, leader)


def draw_cluster_ids(key, part):
    return cluster_layout(key)


def draw_embeddings(key, part):
    clusters = cluster_layout(key)
    total = clusters.shape[0]
    paired, leader = pair_layout(key, clusters)
    k_centre = jax.random.fold_in(jax.random.fold_in(key, 23), 0)
    k_weight = jax.random.fold_in(jax.random.fold_in(key, 23), 1)
    k_noise = jax.random.fold_in(jax.random.fold_in(key, 23), 2)
    k_extra = jax.random.fold_in(jax.random.fold_in(key, 23), 4)
    centres = jax.random.normal(k_centre, (CL_GRP * N_GRP, D), jnp.float32)
    weight = jax.random.uniform(k_weight, (total, 1), jnp.float32, 0.1, 1.0)
    noise = jax.random.normal(k_noise, (total, D), jnp.float32)
    extra = jax.random.normal(k_extra, (total, D), jnp.float32)
    shared = jnp.where(paired[:, None], noise[leader] + 0.2 * extra, noise)
    values = weight * centres[clusters] + shared
    return jnp.clip(values, -60.0, 60.0).astype(jnp.bfloat16)


def setup_inputs(seed: int = 0) -> dict:
    key_list = jax.random.split(jax.random.key(seed), 4)
    embeddings = draw_embeddings(jax.random.fold_in(key_list[3], 71), 0)
    cluster_ids = draw_cluster_ids(jax.random.fold_in(key_list[3], 71), 0)
    rank_key = jax.random.permutation(key_list[2], ROWS).astype(jnp.int32)
    return dict(embeddings=embeddings, cluster_ids=cluster_ids, rank_key=rank_key)


epsilon = 1e-06

def reference(embeddings, cluster_ids, rank_key):
    total = embeddings.shape[0]
    values = embeddings.astype(jnp.float32)
    squares = lax.optimization_barrier(jnp.sum(values * values, axis=1, keepdims=True))
    unit = (values * lax.rsqrt(squares + epsilon)).astype(jnp.bfloat16)
    unit = lax.optimization_barrier(unit).astype(jnp.float32)
    room = 2 * ROWS_DEV * N_BLK
    width = math.gcd(room, 512)
    count = room // width

    def one_group(owner_index):
        member = cluster_ids % N_GRP == owner_index
        pick = jnp.argsort(jnp.where(member, 0, 1).astype(jnp.int32), stable=True)[:room].astype(jnp.int32)
        valid = member[pick]
        group_unit = unit[pick]
        group_cluster = jnp.where(valid, cluster_ids[pick], -1)
        group_rank = rank_key[pick]

        def query_block(index):
            start = (index * width).astype(jnp.int32)
            query = lax.dynamic_slice_in_dim(group_unit, start, width, 0)
            query_cluster = lax.dynamic_slice_in_dim(group_cluster, start, width, 0)
            query_rank = lax.dynamic_slice_in_dim(group_rank, start, width, 0)
            score = jnp.dot(query, group_unit.T, precision=lax.Precision.HIGHEST)
            keep = (query_cluster[:, None] == group_cluster[None, :]) & (group_cluster[None, :] >= 0) & (group_rank[None, :] < query_rank[:, None])
            return lax.optimization_barrier(jnp.max(jnp.where(keep, score, -1.0), axis=1))
        found = lax.map(query_block, jnp.arange(count, dtype=jnp.int32)).reshape(room)
        return (pick, valid, found)
    picks, valids, founds = lax.map(one_group, jnp.arange(N_GRP, dtype=jnp.int32))
    places = jnp.where(valids, picks, total).reshape(-1)
    best = jnp.full((total,), -1.0, jnp.float32)
    return best.at[places].set(founds.reshape(-1), mode='drop')
```

```python
import functools

import jax
import jax.numpy as jnp
from jax import lax
from jax.experimental import pallas as pl
from jax.experimental.pallas import tpu as pltpu
from jax.sharding import PartitionSpec as P

MESH = pl.DeviceIdType.MESH
epsilon = 1e-06
FAR = 1.0e6
OWN, PARTNER, NEXT, CROSS, PREV = range(5)
LAG = 8


def kernel(
    emb_ref, cl_ref, rk_ref, out_ref,
    buf, send, onehot, meta_send, meta_recv, rank_lane, rank_sub, lane_acc, sub_acc,
    part_send, part_recv, final, back_recv,
    meta_s, meta_r, own_s, own_r, rank_s, rank_r, part_s, part_r, back_s, back_r,
    *, groups, members, slot,
):
    rows, depth = emb_ref.shape
    slots = groups * slot
    chips = members // 2
    group, member = lax.axis_index("grp"), lax.axis_index("blk")
    chip, core = member // 2, lax.rem(member, 2)
    after, before = lax.rem(chip + 1, chips), lax.rem(chip + chips - 1, chips)
    partner = {"blk": chip * 2 + 1 - core}
    next_same, next_other = {"blk": after * 2 + core}, {"blk": after * 2 + 1 - core}
    prev_same, prev_other = {"blk": before * 2 + core}, {"blk": before * 2 + 1 - core}

    def ahead(k):
        return {"grp": lax.rem(group + k, groups)}

    def behind(k):
        return {"grp": lax.rem(group + groups - k, groups)}

    barrier = pltpu.get_barrier_semaphore()

    def greet(k, carry):
        pl.semaphore_signal(barrier, inc=1, device_id=ahead(k), device_id_type=MESH)
        return carry

    lax.fori_loop(1, groups, greet, 0)
    for peer in (partner, next_same, next_other, prev_same, prev_other):
        pl.semaphore_signal(barrier, inc=1, device_id=peer, device_id_type=MESH)

    def copy(src, dst, ssem, rsem, peer):
        return pltpu.make_async_remote_copy(
            src_ref=src, dst_ref=dst, send_sem=ssem, recv_sem=rsem,
            device_id=peer, device_id_type=MESH,
        )

    def piece(k):
        return pl.ds(pl.multiple_of(k * slot, slot), slot)

    def exchange(k):
        return copy(send.at[piece(k)], buf.at[OWN, piece(k)], own_s.at[OWN], own_r.at[OWN, k], ahead(k))

    def to_partner(k):
        return copy(buf.at[OWN, piece(k)], buf.at[PARTNER, piece(k)], own_s.at[PARTNER], own_r.at[PARTNER, k], partner)

    def to_prev(k):
        return copy(buf.at[OWN, piece(k)], buf.at[NEXT, piece(k)], own_s.at[NEXT], own_r.at[NEXT, k], prev_same)

    def to_next(k):
        return copy(buf.at[OWN, piece(k)], buf.at[PREV, piece(k)], own_s.at[PREV], own_r.at[PREV, k], next_same)

    def across(k):
        return copy(buf.at[NEXT, piece(k)], buf.at[CROSS, piece(k)], own_s.at[CROSS], own_r.at[CROSS, k], partner)

    def meta(k):
        return copy(meta_send.at[k], meta_recv.at[k], meta_s, meta_r.at[k], ahead(k))

    away = lax.bitwise_and(cl_ref[...] + (groups - group), groups - 1)
    lines = lax.broadcasted_iota(jnp.int32, (groups, rows), 0)
    mine = away == lines
    earlier = lax.broadcasted_iota(jnp.int32, (rows, rows), 0) < lax.broadcasted_iota(jnp.int32, (rows, rows), 1)
    count = jnp.dot(
        jnp.where(mine, 1.0, 0.0).astype(jnp.bfloat16),
        jnp.where(earlier, 1.0, 0.0).astype(jnp.bfloat16),
        preferred_element_type=jnp.float32,
    )
    target = jnp.sum(
        jnp.where(mine, count + (lines * slot).astype(jnp.float32), 0.0), axis=0, keepdims=True
    )
    part = 4 * slot
    for j in range(slots // part):
        at = (lax.broadcasted_iota(jnp.int32, (part, rows), 0) + j * part).astype(jnp.float32)
        onehot[j * part : (j + 1) * part, :] = jnp.where(at == target, 1.0, 0.0).astype(jnp.bfloat16)

    rank = rk_ref[...]
    line8 = lax.broadcasted_iota(jnp.int32, (8, rows), 0)
    high = lax.shift_right_logical(rank, 8).astype(jnp.float32)
    low = lax.bitwise_and(rank, 255).astype(jnp.float32)
    table = jnp.where(line8 == 0, high, jnp.where(line8 == 1, low, 1.0)).astype(jnp.bfloat16)
    found = lax.dot_general(
        table, onehot[...], (((1,), (1,)), ((), ())), preferred_element_type=jnp.float32
    )
    place = found[0:1] * 256.0 + found[1:2] + (1.0 - found[2:3]) * FAR
    left = lax.broadcasted_iota(jnp.int32, (8, 128), 1) < slot
    for t in range(slots // 128):
        tile = jnp.broadcast_to(place[:, t * 128 : (t + 1) * 128], (8, 128))
        turned = pltpu.roll(tile, slot, 1)
        meta_send[2 * t] = jnp.where(left, tile, turned)
        meta_send[2 * t + 1] = jnp.where(left, turned, tile)

    values = emb_ref[...].astype(jnp.float32)
    squares = jnp.sum(values * values, axis=1, keepdims=True)
    unit = (values * lax.rsqrt(squares + epsilon)).astype(jnp.bfloat16)

    for j in range(slots // part):
        packed = jnp.dot(
            onehot[j * part : (j + 1) * part, :], unit, preferred_element_type=jnp.float32
        ).astype(jnp.bfloat16)
        send[j * part : (j + 1) * part, :] = packed
        if j == 0:
            buf[OWN, 0:slot, :] = packed[0:slot]
            pl.semaphore_wait(barrier, groups - 1 + 5)
            for k in range(1, groups):
                meta(k).start()
        for k in range(4 * j, 4 * j + 4):
            if k > 0:
                exchange(k).start()
            else:
                to_prev(0).start()
                to_next(0).start()
                to_partner(0).start()

    lane_acc[...] = jnp.full(lane_acc.shape, -1.0, jnp.float32)
    sub_acc[...] = jnp.full(sub_acc.shape, -1.0, jnp.float32)

    for k in range(1, groups):
        meta(k).wait_recv()
    for t in range(slots // 128):
        first = meta_send[0] if t == 0 else meta_recv[2 * t]
        rank_lane[OWN, t : t + 1, :] = jnp.where(left, first, meta_recv[2 * t + 1])[0:1]
    rank_copies = [
        copy(rank_lane.at[OWN], rank_lane.at[PARTNER], rank_s.at[PARTNER], rank_r.at[PARTNER], partner),
        copy(rank_lane.at[OWN], rank_lane.at[NEXT], rank_s.at[NEXT], rank_r.at[NEXT], prev_same),
        copy(rank_lane.at[OWN], rank_lane.at[PREV], rank_s.at[PREV], rank_r.at[PREV], next_same),
        copy(rank_lane.at[NEXT], rank_lane.at[CROSS], rank_s.at[CROSS], rank_r.at[CROSS], partner),
    ]
    for c in rank_copies[:3]:
        c.start()

    def spread(which):
        for t in range(slots // 128):
            tile = jnp.broadcast_to(rank_lane[which, t : t + 1, :], (128, 128))
            rank_sub[which, t * 128 : (t + 1) * 128, :] = jnp.transpose(tile)

    def relay(k):
        to_prev(k).wait_recv()
        across(k).start()

    def onward(k, carry):
        exchange(k).wait_recv()
        to_prev(k).start()
        to_next(k).start()
        to_partner(k).start()

        @pl.when(k >= LAG)
        def _():
            relay(k - LAG)

        return carry

    half = groups // 2
    lax.fori_loop(1, half, onward, 0)
    spread(OWN)
    rank_copies[0].wait_recv()
    rank_copies[1].wait_recv()
    rank_copies[3].start()
    spread(PARTNER)
    spread(NEXT)
    rank_copies[2].wait_recv()
    rank_copies[3].wait_recv()
    spread(CROSS)
    lax.fori_loop(half, groups, onward, 0)

    def score(x, x0, y, lanes, subs):
        at = pl.ds(x0, part)
        here = rank_sub[x, at, :]
        best = jnp.full((part, 128), -1.0, jnp.float32)
        for n in range(slots // 256):
            s = lax.dot_general(
                buf[x, at, :], buf[y, n * 256 : (n + 1) * 256, :], (((1,), (1,)), ((), ())),
                preferred_element_type=jnp.float32,
            )
            for h in range(2):
                t = 2 * n + h
                sh = s[:, h * 128 : (h + 1) * 128]
                there = rank_lane[y, t : t + 1, :]
                up = jnp.where(here < there, sh, -1.0)
                lane_acc[lanes, t] = jnp.maximum(lane_acc[lanes, t], jnp.max(up.reshape(part // 8, 8, 128), axis=0))
                if subs is not None:
                    best = jnp.maximum(best, jnp.where(there < here, sh, -1.0))
        if subs is not None:
            sub_acc[subs, at, :] = jnp.maximum(sub_acc[subs, at, :], best)

    def square(x, x0, y0):
        here = rank_sub[x, pl.ds(x0, part), :]
        s = lax.dot_general(
            buf[x, pl.ds(x0, part), :], buf[PREV, pl.ds(y0, part), :], (((1,), (1,)), ((), ())),
            preferred_element_type=jnp.float32,
        )
        best = jnp.full((part, 128), -1.0, jnp.float32)
        for h in range(part // 128):
            t = y0 // 128 + h
            sh = s[:, h * 128 : (h + 1) * 128]
            there = rank_lane[PREV, pl.ds(t, 1), :]
            up = jnp.where(here < there, sh, -1.0)
            lane_acc[1, t] = jnp.maximum(lane_acc[1, t], jnp.max(up.reshape(part // 8, 8, 128), axis=0))
            best = jnp.maximum(best, jnp.where(there < here, sh, -1.0))
        at = pl.ds(x0, part)
        sub_acc[x - NEXT, at, :] = jnp.maximum(sub_acc[x - NEXT, at, :], best)

    parts = slots // part
    far = NEXT + chip // (chips // 2)

    def own_rows(i, carry):
        score(OWN, pl.multiple_of(i * part, part), OWN, 0, None)
        return carry

    lax.fori_loop(0, parts, own_rows, 0)

    def take(which):
        def step(k, carry):
            which(k).wait_recv()
            return carry
        return step

    lax.fori_loop(0, groups, take(to_partner), 0)

    def partner_rows(i, carry):
        score(PARTNER, pl.multiple_of(i * part, part), OWN, 0, None)
        return carry

    lax.fori_loop(0, parts, partner_rows, 0)

    def arrived(j, carry):
        @pl.when(j >= LAG // 4)
        def _():
            def step(k, c):
                relay(k)
                return c
            lax.fori_loop(4 * j, 4 * j + 4, step, 0)

        x0 = pl.multiple_of(j * part, part)
        score(NEXT, x0, OWN, 0, 0)
        lax.fori_loop(4 * j, 4 * j + 4, take(across), 0)
        score(CROSS, x0, OWN, 0, 1)
        lax.fori_loop(4 * j, 4 * j + 4, take(to_next), 0)

        def upto(i, c):
            square(far, pl.multiple_of(i * part, part), x0)
            return c

        lax.fori_loop(0, j + 1, upto, 0)

        def below(i, c):
            square(far, x0, pl.multiple_of(i * part, part))
            return c

        lax.fori_loop(0, j, below, 0)
        return carry

    lax.fori_loop(0, parts, arrived, 0)

    for t in range(slots // 128):
        line = slice(t, t + 1)
        for which in range(2):
            tile = jnp.transpose(sub_acc[which, t * 128 : (t + 1) * 128, :])
            part_send[which, line, :] = jnp.max(tile, axis=0, keepdims=True)
        part_send[2, line, :] = jnp.max(lane_acc[1, t], axis=0, keepdims=True)
        final[line, :] = jnp.max(lane_acc[0, t], axis=0, keepdims=True)
    part_copies = [
        copy(part_send.at[i], part_recv.at[i], part_s.at[i], part_r.at[i], peer)
        for i, peer in enumerate((next_same, next_other, prev_same))
    ]
    for c in part_copies:
        c.start()
    for c in part_copies:
        c.wait_recv()
    final[...] = jnp.maximum(
        jnp.maximum(final[...], part_recv[0]), jnp.maximum(part_recv[1], part_recv[2])
    )

    def back(k):
        return copy(final, back_recv.at[k], back_s, back_r.at[k], behind(k))

    for k in range(1, groups):
        back(k).start()
    for k in range(1, groups):
        back(k).wait_recv()
    lines = []
    for t in range(slots // 128):
        line = slice(t, t + 1)
        first = final[line, :] if t == 0 else back_recv[2 * t, line, :]
        lines.append(jnp.where(left[0:1], first, back_recv[2 * t + 1, line, :]))
    got = jnp.concatenate(lines, axis=1)
    one = got.astype(jnp.bfloat16)
    rest = got - one.astype(jnp.float32)
    two = rest.astype(jnp.bfloat16)
    three = rest - two.astype(jnp.float32)
    line8 = lax.broadcasted_iota(jnp.int32, (8, slots), 0)
    terms = jnp.where(
        line8 == 0, one.astype(jnp.float32),
        jnp.where(line8 == 1, two.astype(jnp.float32), jnp.where(line8 == 2, three, 0.0)),
    ).astype(jnp.bfloat16)
    out = jnp.dot(terms, onehot[...], preferred_element_type=jnp.float32)
    out_ref[...] = jnp.sum(out, axis=0, keepdims=True)

    copy(send.at[slot:slots], buf.at[OWN, slot:slots], own_s.at[OWN], own_r.at[OWN, 1], partner).wait_send()
    for which in (PARTNER, NEXT, PREV, CROSS):
        copy(buf.at[OWN], buf.at[which], own_s.at[which], own_r.at[which, 0], partner).wait_send()
    copy(meta_send.at[1:groups], meta_recv.at[1:groups], meta_s, meta_r.at[1], partner).wait_send()
    for c in rank_copies + part_copies:
        c.wait_send()
    copy(meta_send.at[1:groups], back_recv.at[1:groups], back_s, back_r.at[1], partner).wait_send()


def local(embeddings, cluster_ids, rank_key):
    rows, depth = embeddings.shape
    groups, members = lax.axis_size("grp"), lax.axis_size("blk")
    slot = 2 * rows // groups
    slots = groups * slot
    dma = pltpu.SemaphoreType.DMA
    out = pl.pallas_call(
        functools.partial(kernel, groups=groups, members=members, slot=slot),
        out_shape=jax.ShapeDtypeStruct((1, rows), jnp.float32),
        in_specs=[pl.BlockSpec(memory_space=pltpu.VMEM)] * 3,
        out_specs=pl.BlockSpec(memory_space=pltpu.VMEM),
        scratch_shapes=[
            pltpu.VMEM((5, slots, depth), jnp.bfloat16),
            pltpu.VMEM((slots, depth), jnp.bfloat16),
            pltpu.VMEM((slots, rows), jnp.bfloat16),
            pltpu.VMEM((groups, 8, 128), jnp.float32),
            pltpu.VMEM((groups, 8, 128), jnp.float32),
            pltpu.VMEM((5, slots // 128, 128), jnp.float32),
            pltpu.VMEM((4, slots, 128), jnp.float32),
            pltpu.VMEM((2, slots // 128, 8, 128), jnp.float32),
            pltpu.VMEM((2, slots, 128), jnp.float32),
            pltpu.VMEM((3, slots // 128, 128), jnp.float32),
            pltpu.VMEM((3, slots // 128, 128), jnp.float32),
            pltpu.VMEM((slots // 128, 128), jnp.float32),
            pltpu.VMEM((groups, slots // 128, 128), jnp.float32),
            dma, dma((groups,)),
            dma((5,)), dma((5, groups)),
            dma((5,)), dma((5,)),
            dma((3,)), dma((3,)),
            dma, dma((groups,)),
        ],
        compiler_params=pltpu.CompilerParams(
            collective_id=0, has_side_effects=True, vmem_limit_bytes=48 * 1024 * 1024
        ),
    )(embeddings, cluster_ids.reshape(1, rows), rank_key.reshape(1, rows))
    return out.reshape(rows)


def solution(mesh):
    placed = (P(("grp", "blk"), None), P(("grp", "blk")), P(("grp", "blk")))
    return jax.shard_map(
        local, mesh=mesh, in_specs=placed, out_specs=P(("grp", "blk")), check_vma=False
    )
```

```python
import functools

import jax
import jax.numpy as jnp
from jax import lax
from jax.experimental import pallas as pl
from jax.experimental.pallas import tpu as pltpu
from jax.sharding import PartitionSpec as P

MESH = pl.DeviceIdType.MESH
epsilon = 1e-06
FAR = 1.0e6
OWN, PARTNER, NEXT, CROSS, PREV = range(5)
LAG = 6


STEPS = (
    (0, 0), (0, 1), (0, 3), (1, 0), (3, 0), (1, 1), (3, 3), (1, 3),
    (3, 1), (0, 2), (2, 0), (1, 2), (2, 1), (3, 2), (2, 3), (2, 2),
)


def kernel(
    emb_hbm, cl_hbm, rk_hbm, out_ref,
    emb, cl, rk, buf, send, onehot, meta_send, meta_recv, rank_lane, rank_sub, lane_acc, sub_acc,
    part_send, part_recv, final, back_recv,
    in_s, meta_s, meta_r, own_s, own_r, rank_s, rank_r, part_s, part_r, back_s, back_r,
    *, groups, members, slot,
):
    rows, depth = emb.shape
    slots = groups * slot
    tiles = slots // 128
    chips = members // 2
    group, member = lax.axis_index("grp"), lax.axis_index("blk")
    chip, core = member // 2, lax.rem(member, 2)
    after, before = lax.rem(chip + 1, chips), lax.rem(chip + chips - 1, chips)
    partner = {"blk": chip * 2 + 1 - core}
    next_same, next_other = {"blk": after * 2 + core}, {"blk": after * 2 + 1 - core}
    prev_same, prev_other = {"blk": before * 2 + core}, {"blk": before * 2 + 1 - core}
    gz, gx = group // 4, lax.rem(group, 4)

    fetch = [
        pltpu.make_async_copy(cl_hbm, cl, in_s.at[0]),
        pltpu.make_async_copy(emb_hbm, emb, in_s.at[1]),
        pltpu.make_async_copy(rk_hbm, rk, in_s.at[2]),
    ]
    for c in fetch:
        c.start()

    def group_at(k, sign):
        dz, dx = STEPS[k]
        dz, dx = (sign * dz) % 4, (sign * dx) % 4
        return lax.rem(gz + dz, 4) * 4 + lax.rem(gx + dx, 4)

    def ahead(k):
        return {"grp": group_at(k, 1)}

    def behind(k):
        return {"grp": group_at(k, -1)}

    barrier = pltpu.get_barrier_semaphore()
    for k in range(1, groups):
        pl.semaphore_signal(barrier, inc=1, device_id=ahead(k), device_id_type=MESH)
    for peer in (partner, next_same, next_other, prev_same, prev_other):
        pl.semaphore_signal(barrier, inc=1, device_id=peer, device_id_type=MESH)

    def copy(src, dst, ssem, rsem, peer):
        return pltpu.make_async_remote_copy(
            src_ref=src, dst_ref=dst, send_sem=ssem, recv_sem=rsem,
            device_id=peer, device_id_type=MESH,
        )

    def piece(k):
        return pl.ds(k * slot, slot)

    def exchange(k):
        return copy(send.at[piece(k)], buf.at[OWN, piece(k)], own_s.at[OWN], own_r.at[OWN, k], ahead(k))

    def to_partner(k):
        return copy(buf.at[OWN, piece(k)], buf.at[PARTNER, piece(k)], own_s.at[PARTNER], own_r.at[PARTNER, k], partner)

    def to_prev(k):
        return copy(buf.at[OWN, piece(k)], buf.at[NEXT, piece(k)], own_s.at[NEXT], own_r.at[NEXT, k], prev_same)

    def to_next(k):
        return copy(buf.at[OWN, piece(k)], buf.at[PREV, piece(k)], own_s.at[PREV], own_r.at[PREV, k], next_same)

    def across(k):
        return copy(buf.at[NEXT, piece(k)], buf.at[CROSS, piece(k)], own_s.at[CROSS], own_r.at[CROSS, k], partner)

    def meta(k):
        return copy(meta_send.at[k], meta_recv.at[k], meta_s, meta_r.at[k], ahead(k))

    lines = lax.broadcasted_iota(jnp.int32, (groups, rows), 0)
    owner = jnp.full((groups, rows), group, jnp.int32)
    for k in range(1, groups):
        owner = jnp.where(lines == k, group_at(k, 1), owner)
    earlier = lax.broadcasted_iota(jnp.int32, (rows, rows), 0) < lax.broadcasted_iota(jnp.int32, (rows, rows), 1)
    earlier = jnp.where(earlier, 1.0, 0.0).astype(jnp.bfloat16)
    fetch[0].wait()
    mine = lax.bitwise_and(cl[...], groups - 1) == owner
    count = jnp.dot(
        jnp.where(mine, 1.0, 0.0).astype(jnp.bfloat16), earlier, preferred_element_type=jnp.float32
    )
    target = jnp.sum(
        jnp.where(mine, count + (lines * slot).astype(jnp.float32), 0.0), axis=0, keepdims=True
    )
    part = 4 * slot

    def place(j):
        at = (lax.broadcasted_iota(jnp.int32, (part, rows), 0) + j * part).astype(jnp.float32)
        onehot[j * part : (j + 1) * part, :] = jnp.where(at == target, 1.0, 0.0).astype(jnp.bfloat16)

    def pack(j):
        return jnp.dot(
            onehot[j * part : (j + 1) * part, :], unit, preferred_element_type=jnp.float32
        ).astype(jnp.bfloat16)

    place(0)
    fetch[1].wait()
    values = emb[...].astype(jnp.float32)
    squares = jnp.sum(values * values, axis=1, keepdims=True)
    unit = (values * lax.rsqrt(squares + epsilon)).astype(jnp.bfloat16)
    packed = pack(0)
    buf[OWN, 0:slot, :] = packed[0:slot]
    send[0:part, :] = packed
    pl.semaphore_wait(barrier, groups - 1 + 5)
    to_prev(0).start()
    to_next(0).start()
    for k in range(1, 4):
        exchange(k).start()
    to_partner(0).start()

    for j in range(1, slots // part):
        place(j)
    fetch[2].wait()
    rank = rk[...]
    line8 = lax.broadcasted_iota(jnp.int32, (8, rows), 0)
    high = lax.shift_right_logical(rank, 8).astype(jnp.float32)
    low = lax.bitwise_and(rank, 255).astype(jnp.float32)
    table = jnp.where(line8 == 0, high, jnp.where(line8 == 1, low, 1.0)).astype(jnp.bfloat16)
    found = lax.dot_general(
        table, onehot[...], (((1,), (1,)), ((), ())), preferred_element_type=jnp.float32
    )
    spot = found[0:1] * 256.0 + found[1:2] + (1.0 - found[2:3]) * FAR
    left = lax.broadcasted_iota(jnp.int32, (8, 128), 1) < slot
    for t in range(tiles):
        tile = jnp.broadcast_to(spot[:, t * 128 : (t + 1) * 128], (8, 128))
        turned = pltpu.roll(tile, slot, 1)
        meta_send[2 * t] = jnp.where(left, tile, turned)
        meta_send[2 * t + 1] = jnp.where(left, turned, tile)
    for k in range(1, groups):
        meta(k).start()
    for j in range(1, slots // part):
        send[j * part : (j + 1) * part, :] = pack(j)
        for k in range(4 * j, 4 * j + 4):
            exchange(k).start()

    lane_acc[...] = jnp.full(lane_acc.shape, -1.0, jnp.float32)
    sub_acc[...] = jnp.full(sub_acc.shape, -1.0, jnp.float32)

    rank_copies = [
        copy(rank_lane.at[OWN], rank_lane.at[PARTNER], rank_s.at[PARTNER], rank_r.at[PARTNER], partner),
        copy(rank_lane.at[OWN], rank_lane.at[NEXT], rank_s.at[NEXT], rank_r.at[NEXT], prev_same),
        copy(rank_lane.at[OWN], rank_lane.at[PREV], rank_s.at[PREV], rank_r.at[PREV], next_same),
        copy(rank_lane.at[NEXT], rank_lane.at[CROSS], rank_s.at[CROSS], rank_r.at[CROSS], partner),
    ]

    def spread(which, into):
        for t in range(tiles):
            tile = jnp.broadcast_to(rank_lane[which, t : t + 1, :], (128, 128))
            rank_sub[into, t * 128 : (t + 1) * 128, :] = jnp.transpose(tile)

    def relay(k):
        to_prev(k).wait_recv()
        across(k).start()

    def score(x, x0, size, y, y0, width, subs, lanes):
        at = pl.ds(x0, size)
        here = rank_sub[subs, at, :]
        best = jnp.full((size, 128), -1.0, jnp.float32)
        s = lax.dot_general(
            buf[x, at, :], buf[y, pl.ds(y0, width), :], (((1,), (1,)), ((), ())),
            preferred_element_type=jnp.float32,
        )
        for h in range(width // 128):
            t = y0 // 128 + h
            sh = s[:, h * 128 : (h + 1) * 128]
            there = rank_lane[y, pl.ds(t, 1), :]
            best = jnp.maximum(best, jnp.where(there < here, sh, -1.0))
            if lanes is not None:
                up = jnp.where(here < there, sh, -1.0)
                lane_acc[lanes, t] = jnp.maximum(lane_acc[lanes, t], jnp.max(up.reshape(size // 8, 8, 128), axis=0))
        sub_acc[subs, at, :] = jnp.maximum(sub_acc[subs, at, :], best)

    def each(first, last, body):
        def step(i, carry):
            body(i)
            return carry
        lax.fori_loop(first, last, step, 0)

    far = NEXT + chip // (chips // 2)

    def chunk(i):
        return pl.multiple_of(i * part, part)

    for k in range(1, groups):
        exchange(k).wait_recv()
        to_prev(k).start()
        to_next(k).start()
        to_partner(k).start()
        if k >= LAG:
            relay(k - LAG)
        if k == 4:
            for i in range(1, groups):
                meta(i).wait_recv()
            for t in range(tiles):
                first = meta_send[0] if t == 0 else meta_recv[2 * t]
                rank_lane[OWN, t : t + 1, :] = jnp.where(left, first, meta_recv[2 * t + 1])[0:1]
            for c in rank_copies[:3]:
                c.start()
            spread(OWN, 0)
        if k == 8:
            for c in rank_copies[:3]:
                c.wait_recv()
            rank_copies[3].start()
            spread(PREV, 1)
        if k == 9:
            for j in range(2):
                score(OWN, 0, (j + 1) * part, OWN, j * part, part, 0, 0)
        if k == 10:
            for i in range(8):
                to_partner(i).wait_recv()
            each(0, 2, lambda i: score(OWN, 0, 2 * part, PARTNER, chunk(i), part, 0, None))
        if k == 13:
            score(OWN, 0, 3 * part, OWN, 2 * part, part, 0, 0)

    score(OWN, 0, slots, OWN, 3 * part, part, 0, 0)
    relay(16 - LAG)
    each(0, 2, lambda i: score(OWN, 2 * part, 2 * part, PARTNER, chunk(i), part, 0, None))
    for i in range(8, 16):
        to_partner(i).wait_recv()
    relay(17 - LAG)
    each(2, 4, lambda i: score(OWN, 0, slots, PARTNER, chunk(i), part, 0, None))
    rank_copies[3].wait_recv()

    sent = 18 - LAG
    for j in range(slots // part):
        now = j * part
        while sent < 4 * j + 4:
            relay(sent)
            sent += 1
        score(OWN, 0, slots, NEXT, now, part, 0, NEXT)
        for k in range(4 * j, 4 * j + 4):
            across(k).wait_recv()
            to_next(k).wait_recv()
        score(OWN, 0, slots, CROSS, now, part, 0, CROSS)
        if j == 1:
            each(0, 2, lambda i: score(PREV, 0, 2 * part, far, chunk(i), part, 1, far))
        if j >= 2:
            score(PREV, 0, now + part, far, now, part, 1, far)
            each(0, j, lambda i: score(PREV, now, part, far, chunk(i), part, 1, far))

    for t in range(tiles):
        line = slice(t, t + 1)
        for i, which in enumerate((NEXT, CROSS)):
            part_send[i, line, :] = jnp.max(lane_acc[which, t], axis=0, keepdims=True)
        tile = jnp.transpose(sub_acc[1, t * 128 : (t + 1) * 128, :])
        part_send[2, line, :] = jnp.max(tile, axis=0, keepdims=True)
    part_copies = [
        copy(part_send.at[i], part_recv.at[i], part_s.at[i], part_r.at[i], peer)
        for i, peer in enumerate((next_same, next_other, prev_same))
    ]
    for c in part_copies:
        c.start()
    for t in range(tiles):
        tile = jnp.maximum(jnp.transpose(sub_acc[0, t * 128 : (t + 1) * 128, :]), jnp.max(lane_acc[0, t], axis=0, keepdims=True))
        final[t : t + 1, :] = jnp.max(tile, axis=0, keepdims=True)
    for c in part_copies:
        c.wait_recv()
    final[...] = jnp.maximum(
        jnp.maximum(final[...], part_recv[0]), jnp.maximum(part_recv[1], part_recv[2])
    )

    def back(k):
        return copy(final, back_recv.at[k], back_s, back_r.at[k], behind(k))

    for k in range(1, groups):
        back(k).start()
    for k in range(1, groups):
        back(k).wait_recv()
    found = []
    for t in range(tiles):
        line = slice(t, t + 1)
        first = final[line, :] if t == 0 else back_recv[2 * t, line, :]
        found.append(jnp.where(left[0:1], first, back_recv[2 * t + 1, line, :]))
    got = jnp.concatenate(found, axis=1)
    one = got.astype(jnp.bfloat16).astype(jnp.float32)
    rest = got - one
    two = rest.astype(jnp.bfloat16).astype(jnp.float32)
    line8 = lax.broadcasted_iota(jnp.int32, (8, slots), 0)
    terms = jnp.where(
        line8 == 0, one, jnp.where(line8 == 1, two, jnp.where(line8 == 2, rest - two, 0.0))
    ).astype(jnp.bfloat16)
    out = jnp.dot(terms, onehot[...], preferred_element_type=jnp.float32)
    out_ref[...] = jnp.sum(out, axis=0, keepdims=True)

    copy(send.at[slot:slots], buf.at[OWN, slot:slots], own_s.at[OWN], own_r.at[OWN, 1], partner).wait_send()
    for which in (PARTNER, NEXT, PREV, CROSS):
        copy(buf.at[OWN], buf.at[which], own_s.at[which], own_r.at[which, 0], partner).wait_send()
    copy(meta_send.at[1:groups], meta_recv.at[1:groups], meta_s, meta_r.at[1], partner).wait_send()
    for c in rank_copies + part_copies:
        c.wait_send()
    copy(meta_send.at[1:groups], back_recv.at[1:groups], back_s, back_r.at[1], partner).wait_send()


def local(embeddings, cluster_ids, rank_key):
    rows, depth = embeddings.shape
    groups, members = lax.axis_size("grp"), lax.axis_size("blk")
    slot = 2 * rows // groups
    slots = groups * slot
    dma = pltpu.SemaphoreType.DMA
    out = pl.pallas_call(
        functools.partial(kernel, groups=groups, members=members, slot=slot),
        out_shape=jax.ShapeDtypeStruct((1, rows), jnp.float32),
        in_specs=[pl.BlockSpec(memory_space=pltpu.HBM)] * 3,
        out_specs=pl.BlockSpec(memory_space=pltpu.VMEM),
        scratch_shapes=[
            pltpu.VMEM((rows, depth), jnp.bfloat16),
            pltpu.VMEM((1, rows), jnp.int32),
            pltpu.VMEM((1, rows), jnp.int32),
            pltpu.VMEM((5, slots, depth), jnp.bfloat16),
            pltpu.VMEM((slots, depth), jnp.bfloat16),
            pltpu.VMEM((slots, rows), jnp.bfloat16),
            pltpu.VMEM((groups, 8, 128), jnp.float32),
            pltpu.VMEM((groups, 8, 128), jnp.float32),
            pltpu.VMEM((5, slots // 128, 128), jnp.float32),
            pltpu.VMEM((2, slots, 128), jnp.float32),
            pltpu.VMEM((4, slots // 128, 8, 128), jnp.float32),
            pltpu.VMEM((2, slots, 128), jnp.float32),
            pltpu.VMEM((3, slots // 128, 128), jnp.float32),
            pltpu.VMEM((3, slots // 128, 128), jnp.float32),
            pltpu.VMEM((slots // 128, 128), jnp.float32),
            pltpu.VMEM((groups, slots // 128, 128), jnp.float32),
            dma((3,)),
            dma, dma((groups,)),
            dma((5,)), dma((5, groups)),
            dma((5,)), dma((5,)),
            dma((3,)), dma((3,)),
            dma, dma((groups,)),
        ],
        compiler_params=pltpu.CompilerParams(
            collective_id=0, has_side_effects=True, vmem_limit_bytes=48 * 1024 * 1024
        ),
    )(embeddings, cluster_ids.reshape(1, rows), rank_key.reshape(1, rows))
    return out.reshape(rows)


def solution(mesh):
    placed = (P(("grp", "blk"), None), P(("grp", "blk")), P(("grp", "blk")))
    return jax.shard_map(
        local, mesh=mesh, in_specs=placed, out_specs=P(("grp", "blk")), check_vma=False
    )
```

```python
import functools

import jax
import jax.numpy as jnp
from jax import lax
from jax.experimental import pallas as pl
from jax.experimental.pallas import tpu as pltpu
from jax.sharding import PartitionSpec as P

MESH = pl.DeviceIdType.MESH
epsilon = 1e-06
FAR = 1.0e6
OWN, PARTNER, NEXT, PREV = range(4)


STEPS = (
    (0, 0), (0, 1), (0, 3), (1, 0), (3, 0), (1, 1), (3, 3), (1, 3),
    (3, 1), (0, 2), (2, 0), (1, 2), (2, 1), (3, 2), (2, 3), (2, 2),
)


def kernel(
    emb_hbm, cl_hbm, rk_hbm, out_ref,
    emb, cl, rk, buf, send, onehot, meta_send, meta_recv, rank_lane, rank_sub, lane_acc, sub_acc,
    result, returned,
    in_s, meta_s, meta_r, own_s, own_r, rank_s, rank_r, back_s, back_r,
    *, groups, members, slot,
):
    rows, depth = emb.shape
    slots = groups * slot
    tiles = slots // 128
    chips = members // 2
    group, member = lax.axis_index("grp"), lax.axis_index("blk")
    chip, core = member // 2, lax.rem(member, 2)
    after, before = lax.rem(chip + 1, chips), lax.rem(chip + chips - 1, chips)
    partner = {"blk": chip * 2 + 1 - core}
    next_same, next_other = {"blk": after * 2 + core}, {"blk": after * 2 + 1 - core}
    crossed = after // (chips // 2)
    next_seen = {"blk": after * 2 + lax.rem(core + crossed, 2)}
    prev_seen = {"blk": before * 2 + lax.rem(core + chip // (chips // 2), 2)}
    prev_same, prev_other = {"blk": before * 2 + core}, {"blk": before * 2 + 1 - core}
    gz, gx = group // 4, lax.rem(group, 4)

    fetch = [
        pltpu.make_async_copy(cl_hbm, cl, in_s.at[0]),
        pltpu.make_async_copy(emb_hbm, emb, in_s.at[1]),
        pltpu.make_async_copy(rk_hbm, rk, in_s.at[2]),
    ]
    for c in fetch:
        c.start()

    def group_at(k, sign):
        dz, dx = STEPS[k]
        dz, dx = (sign * dz) % 4, (sign * dx) % 4
        return lax.rem(gz + dz, 4) * 4 + lax.rem(gx + dx, 4)

    def ahead(k):
        return {"grp": group_at(k, 1)}

    def behind(k):
        return {"grp": group_at(k, -1)}

    barrier = pltpu.get_barrier_semaphore()
    for k in range(1, groups):
        pl.semaphore_signal(barrier, inc=1, device_id=ahead(k), device_id_type=MESH)
    for peer in (partner, next_same, next_other, prev_same, prev_other):
        pl.semaphore_signal(barrier, inc=1, device_id=peer, device_id_type=MESH)

    def copy(src, dst, ssem, rsem, peer):
        return pltpu.make_async_remote_copy(
            src_ref=src, dst_ref=dst, send_sem=ssem, recv_sem=rsem,
            device_id=peer, device_id_type=MESH,
        )

    def piece(k):
        return pl.ds(k * slot, slot)

    def exchange(k):
        return copy(send.at[piece(k)], buf.at[OWN, piece(k)], own_s.at[OWN], own_r.at[OWN, k], ahead(k))

    def to_partner(k):
        return copy(buf.at[OWN, piece(k)], buf.at[PARTNER, piece(k)], own_s.at[PARTNER], own_r.at[PARTNER, k], partner)

    def to_prev(k):
        return copy(buf.at[OWN, piece(k)], buf.at[NEXT, piece(k)], own_s.at[NEXT], own_r.at[NEXT, k], prev_same)

    def to_next(k):
        return copy(buf.at[OWN, piece(k)], buf.at[PREV, piece(k)], own_s.at[PREV], own_r.at[PREV, k], next_seen)

    def meta(k):
        return copy(meta_send.at[k], meta_recv.at[k], meta_s, meta_r.at[k], ahead(k))

    lines = lax.broadcasted_iota(jnp.int32, (groups, rows), 0)
    owner = jnp.full((groups, rows), group, jnp.int32)
    for k in range(1, groups):
        owner = jnp.where(lines == k, group_at(k, 1), owner)
    earlier = lax.broadcasted_iota(jnp.int32, (rows, rows), 0) < lax.broadcasted_iota(jnp.int32, (rows, rows), 1)
    earlier = jnp.where(earlier, 1.0, 0.0).astype(jnp.bfloat16)
    fetch[0].wait()
    mine = lax.bitwise_and(cl[...], groups - 1) == owner
    count = jnp.dot(
        jnp.where(mine, 1.0, 0.0).astype(jnp.bfloat16), earlier, preferred_element_type=jnp.float32
    )
    target = jnp.sum(
        jnp.where(mine, count + (lines * slot).astype(jnp.float32), 0.0), axis=0, keepdims=True
    )
    part = 4 * slot

    def place(j):
        at = (lax.broadcasted_iota(jnp.int32, (part, rows), 0) + j * part).astype(jnp.float32)
        onehot[j * part : (j + 1) * part, :] = jnp.where(at == target, 1.0, 0.0).astype(jnp.bfloat16)

    def pack(j):
        return jnp.dot(
            onehot[j * part : (j + 1) * part, :], unit, preferred_element_type=jnp.float32
        ).astype(jnp.bfloat16)

    place(0)
    fetch[1].wait()
    values = emb[...].astype(jnp.float32)
    squares = jnp.sum(values * values, axis=1, keepdims=True)
    unit = (values * lax.rsqrt(squares + epsilon)).astype(jnp.bfloat16)
    packed = pack(0)
    buf[OWN, 0:slot, :] = packed[0:slot]
    send[0:part, :] = packed
    pl.semaphore_wait(barrier, groups - 1 + 5)
    to_prev(0).start()
    to_next(0).start()
    for k in range(1, 4):
        exchange(k).start()
    to_partner(0).start()

    for j in range(1, slots // part):
        place(j)
    fetch[2].wait()
    rank = rk[...]
    line8 = lax.broadcasted_iota(jnp.int32, (8, rows), 0)
    high = lax.shift_right_logical(rank, 8).astype(jnp.float32)
    low = lax.bitwise_and(rank, 255).astype(jnp.float32)
    table = jnp.where(line8 == 0, high, jnp.where(line8 == 1, low, 1.0)).astype(jnp.bfloat16)
    found = lax.dot_general(
        table, onehot[...], (((1,), (1,)), ((), ())), preferred_element_type=jnp.float32
    )
    spot = found[0:1] * 256.0 + found[1:2] + (1.0 - found[2:3]) * FAR
    left = lax.broadcasted_iota(jnp.int32, (8, 128), 1) < slot
    for t in range(tiles):
        tile = jnp.broadcast_to(spot[:, t * 128 : (t + 1) * 128], (8, 128))
        turned = pltpu.roll(tile, slot, 1)
        meta_send[2 * t] = jnp.where(left, tile, turned)
        meta_send[2 * t + 1] = jnp.where(left, turned, tile)
    for k in range(1, groups):
        meta(k).start()
    for j in range(1, slots // part):
        send[j * part : (j + 1) * part, :] = pack(j)
        for k in range(4 * j, 4 * j + 4):
            exchange(k).start()

    lane_acc[...] = jnp.full(lane_acc.shape, -1.0, jnp.float32)
    sub_acc[...] = jnp.full(sub_acc.shape, -1.0, jnp.float32)

    rank_copies = [
        copy(rank_lane.at[OWN], rank_lane.at[PARTNER], rank_s.at[PARTNER], rank_r.at[PARTNER], partner),
        copy(rank_lane.at[OWN], rank_lane.at[NEXT], rank_s.at[NEXT], rank_r.at[NEXT], prev_same),
        copy(rank_lane.at[OWN], rank_lane.at[PREV], rank_s.at[PREV], rank_r.at[PREV], next_seen),
    ]

    def spread(which):
        for t in range(tiles):
            tile = jnp.broadcast_to(rank_lane[which, t : t + 1, :], (128, 128))
            rank_sub[which, t * 128 : (t + 1) * 128, :] = jnp.transpose(tile)

    def score(x, x0, size, y, y0, width):
        at = pl.ds(x0, size)
        here = rank_sub[x, at, :]
        best = jnp.full((size, 128), -1.0, jnp.float32)
        s = lax.dot_general(
            buf[x, at, :], buf[y, pl.ds(y0, width), :], (((1,), (1,)), ((), ())),
            preferred_element_type=jnp.float32,
        )
        for h in range(width // 128):
            t = y0 // 128 + h
            sh = s[:, h * 128 : (h + 1) * 128]
            there = rank_lane[y, pl.ds(t, 1), :]
            best = jnp.maximum(best, jnp.where(there < here, sh, -1.0))
            up = jnp.where(here < there, sh, -1.0)
            lane_acc[y, t] = jnp.maximum(lane_acc[y, t], jnp.max(up.reshape(size // 8, 8, 128), axis=0))
        sub_acc[x, at, :] = jnp.maximum(sub_acc[x, at, :], best)

    def each(first, last, body):
        def step(i, carry):
            body(i)
            return carry
        lax.fori_loop(first, last, step, 0)

    def chunk(i):
        return pl.multiple_of(i * part, part)

    for k in range(1, groups):
        exchange(k).wait_recv()
        to_prev(k).start()
        to_next(k).start()
        to_partner(k).start()
        if k == 4:
            for i in range(1, groups):
                meta(i).wait_recv()
            for t in range(tiles):
                first = meta_send[0] if t == 0 else meta_recv[2 * t]
                rank_lane[OWN, t : t + 1, :] = jnp.where(left, first, meta_recv[2 * t + 1])[0:1]
            for c in rank_copies:
                c.start()
            spread(OWN)
        if k == 10:
            for c in rank_copies:
                c.wait_recv()
            spread(PARTNER)

    for j in range(slots // part):
        score(OWN, 0, (j + 1) * part, OWN, j * part, part)
    spread(PREV)
    for k in range(groups):
        to_partner(k).wait_recv()
    each(0, 2, lambda i: score(core, 0, slots, 1 - core, pl.multiple_of(core * 2 * part + i * part, part), part))

    last = slots // part - 1
    for j in range(last):
        now = j * part
        for k in range(4 * j, 4 * j + 4):
            to_prev(k).wait_recv()
        score(OWN, 0, slots, NEXT, now, part)
        score(PARTNER, 0, slots, NEXT, now, part)
        for k in range(4 * j, 4 * j + 4):
            to_next(k).wait_recv()
        if j == 1:
            each(0, 2, lambda i: score(PREV, 0, 2 * part, NEXT, chunk(i), part))
        if j >= 2:
            score(PREV, now, part, NEXT, 0, now)
            score(PREV, 0, now + part, NEXT, now, part)

    def gather(which, t):
        tile = jnp.transpose(sub_acc[which, t * 128 : (t + 1) * 128, :])
        return jnp.max(tile, axis=0, keepdims=True)

    def along(which, t):
        return jnp.max(lane_acc[which, t], axis=0, keepdims=True)

    homes = {PREV: prev_seen, PARTNER: partner, NEXT: next_same, OWN: {}}

    def back(which, k):
        return copy(
            result.at[which, k // 2], returned.at[which, k], back_s.at[which], back_r.at[which],
            {**behind(k), **homes[which]},
        )

    def send_back(which):
        for k in range(1 if which == OWN else 0, groups):
            back(which, k).start()

    now = last * part
    for k in range(4 * last, 4 * last + 4):
        to_next(k).wait_recv()
    for k in range(4 * last, 4 * last + 4):
        to_prev(k).wait_recv()
    score(PREV, now, part, NEXT, 0, now)
    score(PREV, 0, now + part, NEXT, now, part)
    for t in range(tiles):
        result[PREV, t] = gather(PREV, t)
    score(PARTNER, 0, slots, NEXT, now, part)
    send_back(PREV)
    for t in range(tiles):
        result[PARTNER, t] = jnp.maximum(gather(PARTNER, t), along(PARTNER, t))
    score(OWN, 0, slots, NEXT, now, part)
    for t in range(tiles):
        result[NEXT, t] = along(NEXT, t)
    send_back(NEXT)
    send_back(PARTNER)
    for t in range(tiles):
        result[OWN, t] = jnp.maximum(gather(OWN, t), along(OWN, t))
    send_back(OWN)

    def all_back(which):
        first = 1 if which == OWN else 0
        return copy(
            returned.at[which, first:groups], returned.at[which, first:groups],
            back_s.at[which], back_r.at[which], partner,
        )

    for which in (OWN, PARTNER, NEXT, PREV):
        all_back(which).wait_recv()
    found = []
    for t in range(tiles):
        pair = []
        for k in (2 * t, 2 * t + 1):
            one = result[OWN, 0] if k == 0 else returned[OWN, k]
            for which in (PARTNER, NEXT, PREV):
                one = jnp.maximum(one, returned[which, k])
            pair.append(one)
        found.append(jnp.where(left[0:1], pair[0], pair[1]))
    got = jnp.concatenate(found, axis=1)
    one = got.astype(jnp.bfloat16).astype(jnp.float32)
    rest = got - one
    two = rest.astype(jnp.bfloat16).astype(jnp.float32)
    line8 = lax.broadcasted_iota(jnp.int32, (8, slots), 0)
    terms = jnp.where(
        line8 == 0, one, jnp.where(line8 == 1, two, jnp.where(line8 == 2, rest - two, 0.0))
    ).astype(jnp.bfloat16)
    out = jnp.dot(terms, onehot[...], preferred_element_type=jnp.float32)
    out_ref[...] = jnp.sum(out, axis=0, keepdims=True)

    copy(send.at[slot:slots], buf.at[OWN, slot:slots], own_s.at[OWN], own_r.at[OWN, 1], partner).wait_send()
    for which in (PARTNER, NEXT, PREV):
        copy(buf.at[OWN], buf.at[which], own_s.at[which], own_r.at[which, 0], partner).wait_send()
    copy(meta_send.at[1:groups], meta_recv.at[1:groups], meta_s, meta_r.at[1], partner).wait_send()
    for c in rank_copies:
        c.wait_send()
    for which in (OWN, PARTNER, NEXT, PREV):
        all_back(which).wait_send()


def local(embeddings, cluster_ids, rank_key):
    rows, depth = embeddings.shape
    groups, members = lax.axis_size("grp"), lax.axis_size("blk")
    slot = 2 * rows // groups
    slots = groups * slot
    dma = pltpu.SemaphoreType.DMA
    out = pl.pallas_call(
        functools.partial(kernel, groups=groups, members=members, slot=slot),
        out_shape=jax.ShapeDtypeStruct((1, rows), jnp.float32),
        in_specs=[pl.BlockSpec(memory_space=pltpu.HBM)] * 3,
        out_specs=pl.BlockSpec(memory_space=pltpu.VMEM),
        scratch_shapes=[
            pltpu.VMEM((rows, depth), jnp.bfloat16),
            pltpu.VMEM((1, rows), jnp.int32),
            pltpu.VMEM((1, rows), jnp.int32),
            pltpu.VMEM((4, slots, depth), jnp.bfloat16),
            pltpu.VMEM((slots, depth), jnp.bfloat16),
            pltpu.VMEM((slots, rows), jnp.bfloat16),
            pltpu.VMEM((groups, 8, 128), jnp.float32),
            pltpu.VMEM((groups, 8, 128), jnp.float32),
            pltpu.VMEM((4, slots // 128, 128), jnp.float32),
            pltpu.VMEM((4, slots, 128), jnp.float32),
            pltpu.VMEM((4, slots // 128, 8, 128), jnp.float32),
            pltpu.VMEM((4, slots, 128), jnp.float32),
            pltpu.VMEM((4, slots // 128, 1, 128), jnp.float32),
            pltpu.VMEM((4, groups, 1, 128), jnp.float32),
            dma((3,)),
            dma, dma((groups,)),
            dma((4,)), dma((4, groups)),
            dma((4,)), dma((4,)),
            dma((4,)), dma((4,)),
        ],
        compiler_params=pltpu.CompilerParams(
            collective_id=0, has_side_effects=True, vmem_limit_bytes=48 * 1024 * 1024
        ),
    )(embeddings, cluster_ids.reshape(1, rows), rank_key.reshape(1, rows))
    return out.reshape(rows)


def solution(mesh):
    placed = (P(("grp", "blk"), None), P(("grp", "blk")), P(("grp", "blk")))
    return jax.shard_map(
        local, mesh=mesh, in_specs=placed, out_specs=P(("grp", "blk")), check_vma=False
    )
```

```python
import functools

import jax
import jax.numpy as jnp
from jax import lax
from jax.experimental import pallas as pl
from jax.experimental.pallas import tpu as pltpu
from jax.sharding import PartitionSpec as P

MESH = pl.DeviceIdType.MESH
epsilon = 1e-06
FAR = 1.0e6
OWN, PARTNER, NEXT, PREV = range(4)
EARLY, CUT = 2, 2


STEPS = (
    (0, 0), (0, 1), (0, 3), (1, 0), (3, 0), (1, 1), (3, 3), (1, 3),
    (3, 1), (0, 2), (2, 0), (1, 2), (2, 1), (3, 2), (2, 3), (2, 2),
)


def kernel(
    emb_hbm, cl_hbm, rk_hbm, out_ref,
    emb, cl, rk, buf, send, onehot, meta_send, meta_recv, rank_lane, rank_sub, lane_acc, sub_acc,
    result, returned,
    in_s, meta_s, meta_r, own_s, own_r, rank_s, rank_r, back_s, back_r, early_r,
    *, groups, members, slot,
):
    rows, depth = emb.shape
    slots = groups * slot
    tiles = slots // 128
    chips = members // 2
    group, member = lax.axis_index("grp"), lax.axis_index("blk")
    chip, core = member // 2, lax.rem(member, 2)
    after, before = lax.rem(chip + 1, chips), lax.rem(chip + chips - 1, chips)
    partner = {"blk": chip * 2 + 1 - core}
    next_same, next_other = {"blk": after * 2 + core}, {"blk": after * 2 + 1 - core}
    crossed = after // (chips // 2)
    next_seen = {"blk": after * 2 + lax.rem(core + crossed, 2)}
    prev_seen = {"blk": before * 2 + lax.rem(core + chip // (chips // 2), 2)}
    prev_same, prev_other = {"blk": before * 2 + core}, {"blk": before * 2 + 1 - core}
    gz, gx = group // 4, lax.rem(group, 4)

    fetch = [
        pltpu.make_async_copy(cl_hbm, cl, in_s.at[0]),
        pltpu.make_async_copy(emb_hbm, emb, in_s.at[1]),
        pltpu.make_async_copy(rk_hbm, rk, in_s.at[2]),
    ]
    for c in fetch:
        c.start()

    def group_at(k, sign):
        dz, dx = STEPS[k]
        dz, dx = (sign * dz) % 4, (sign * dx) % 4
        return lax.rem(gz + dz, 4) * 4 + lax.rem(gx + dx, 4)

    def ahead(k):
        return {"grp": group_at(k, 1)}

    def behind(k):
        return {"grp": group_at(k, -1)}

    barrier = pltpu.get_barrier_semaphore()
    for k in range(1, groups):
        pl.semaphore_signal(barrier, inc=1, device_id=ahead(k), device_id_type=MESH)
    for peer in (partner, next_same, next_other, prev_same, prev_other):
        pl.semaphore_signal(barrier, inc=1, device_id=peer, device_id_type=MESH)

    def copy(src, dst, ssem, rsem, peer):
        return pltpu.make_async_remote_copy(
            src_ref=src, dst_ref=dst, send_sem=ssem, recv_sem=rsem,
            device_id=peer, device_id_type=MESH,
        )

    def piece(k):
        return pl.ds(k * slot, slot)

    def exchange(k):
        return copy(send.at[piece(k)], buf.at[OWN, piece(k)], own_s.at[OWN], own_r.at[OWN, k], ahead(k))

    def some(k, i):
        return pl.ds(k * slot + i * (slot // CUT), slot // CUT)

    def exchange_some(k, i):
        return copy(send.at[some(k, i)], buf.at[OWN, some(k, i)], own_s.at[OWN], early_r.at[k, i], ahead(k))

    def to_prev_some(k, i):
        return copy(buf.at[OWN, some(k, i)], buf.at[NEXT, some(k, i)], own_s.at[NEXT], own_r.at[NEXT, k], prev_same)

    def to_next_some(k, i):
        return copy(buf.at[OWN, some(k, i)], buf.at[PREV, some(k, i)], own_s.at[PREV], own_r.at[PREV, k], next_seen)

    def to_partner(k):
        return copy(buf.at[OWN, piece(k)], buf.at[PARTNER, piece(k)], own_s.at[PARTNER], own_r.at[PARTNER, k], partner)

    def to_prev(k):
        return copy(buf.at[OWN, piece(k)], buf.at[NEXT, piece(k)], own_s.at[NEXT], own_r.at[NEXT, k], prev_same)

    def to_next(k):
        return copy(buf.at[OWN, piece(k)], buf.at[PREV, piece(k)], own_s.at[PREV], own_r.at[PREV, k], next_seen)

    def meta(k):
        return copy(meta_send.at[k], meta_recv.at[k], meta_s, meta_r.at[k], ahead(k))

    lines = lax.broadcasted_iota(jnp.int32, (groups, rows), 0)
    owner = jnp.full((groups, rows), group, jnp.int32)
    for k in range(1, groups):
        owner = jnp.where(lines == k, group_at(k, 1), owner)
    earlier = lax.broadcasted_iota(jnp.int32, (rows, rows), 0) < lax.broadcasted_iota(jnp.int32, (rows, rows), 1)
    earlier = jnp.where(earlier, 1.0, 0.0).astype(jnp.bfloat16)
    fetch[0].wait()
    fetch[1].wait()
    mine = lax.bitwise_and(cl[...], groups - 1) == owner
    count = jnp.dot(
        jnp.where(mine, 1.0, 0.0).astype(jnp.bfloat16), earlier, preferred_element_type=jnp.float32
    )
    target = jnp.sum(
        jnp.where(mine, count + (lines * slot).astype(jnp.float32), 0.0), axis=0, keepdims=True
    )
    part = 4 * slot

    def place(j):
        at = (lax.broadcasted_iota(jnp.int32, (part, rows), 0) + j * part).astype(jnp.float32)
        onehot[j * part : (j + 1) * part, :] = jnp.where(at == target, 1.0, 0.0).astype(jnp.bfloat16)

    def pack(j):
        return jnp.dot(
            onehot[j * part : (j + 1) * part, :], unit, preferred_element_type=jnp.float32
        ).astype(jnp.bfloat16)

    place(0)
    values = emb[...].astype(jnp.float32)
    squares = jnp.sum(values * values, axis=1, keepdims=True)
    unit = (values * lax.rsqrt(squares + epsilon)).astype(jnp.bfloat16)
    packed = pack(0)
    buf[OWN, 0:slot, :] = packed[0:slot]
    send[0:part, :] = packed
    pl.semaphore_wait(barrier, groups - 1 + 5)
    for i in range(CUT):
        for k in range(1, EARLY + 1):
            exchange_some(k, i).start()
        if i == 0:
            to_prev(0).start()
            to_next(0).start()
    for k in range(EARLY + 1, 4):
        exchange(k).start()
    to_partner(0).start()

    def give(j):
        send[j * part : (j + 1) * part, :] = pack(j)
        for k in range(4 * j, 4 * j + 4):
            exchange(k).start()

    place(1)
    give(1)
    for j in range(2, slots // part):
        place(j)
    fetch[2].wait()
    rank = rk[...]
    line8 = lax.broadcasted_iota(jnp.int32, (8, rows), 0)
    high = lax.shift_right_logical(rank, 8).astype(jnp.float32)
    low = lax.bitwise_and(rank, 255).astype(jnp.float32)
    table = jnp.where(line8 == 0, high, jnp.where(line8 == 1, low, 1.0)).astype(jnp.bfloat16)
    found = lax.dot_general(
        table, onehot[...], (((1,), (1,)), ((), ())), preferred_element_type=jnp.float32
    )
    spot = found[0:1] * 256.0 + found[1:2] + (1.0 - found[2:3]) * FAR
    left = lax.broadcasted_iota(jnp.int32, (8, 128), 1) < slot
    for t in range(tiles):
        tile = jnp.broadcast_to(spot[:, t * 128 : (t + 1) * 128], (8, 128))
        turned = pltpu.roll(tile, slot, 1)
        meta_send[2 * t] = jnp.where(left, tile, turned)
        meta_send[2 * t + 1] = jnp.where(left, turned, tile)
    for k in range(1, groups):
        meta(k).start()
    for j in range(2, slots // part):
        give(j)

    lane_acc[...] = jnp.full(lane_acc.shape, -1.0, jnp.float32)
    sub_acc[...] = jnp.full(sub_acc.shape, -1.0, jnp.float32)

    rank_copies = [
        copy(rank_lane.at[OWN], rank_lane.at[PARTNER], rank_s.at[PARTNER], rank_r.at[PARTNER], partner),
        copy(rank_lane.at[OWN], rank_lane.at[NEXT], rank_s.at[NEXT], rank_r.at[NEXT], prev_same),
        copy(rank_lane.at[OWN], rank_lane.at[PREV], rank_s.at[PREV], rank_r.at[PREV], next_seen),
    ]

    def spread(which):
        for t in range(tiles):
            tile = jnp.broadcast_to(rank_lane[which, t : t + 1, :], (128, 128))
            rank_sub[which, t * 128 : (t + 1) * 128, :] = jnp.transpose(tile)

    def score(x, x0, size, y, y0, width):
        at = pl.ds(x0, size)
        here = rank_sub[x, at, :]
        best = jnp.full((size, 128), -1.0, jnp.float32)
        s = lax.dot_general(
            buf[x, at, :], buf[y, pl.ds(y0, width), :], (((1,), (1,)), ((), ())),
            preferred_element_type=jnp.float32,
        )
        for h in range(width // 128):
            t = y0 // 128 + h
            sh = s[:, h * 128 : (h + 1) * 128]
            there = rank_lane[y, pl.ds(t, 1), :]
            best = jnp.maximum(best, jnp.where(there < here, sh, -1.0))
            up = jnp.where(here < there, sh, -1.0)
            lane_acc[y, t] = jnp.maximum(lane_acc[y, t], jnp.max(up.reshape(size // 8, 8, 128), axis=0))
        sub_acc[x, at, :] = jnp.maximum(sub_acc[x, at, :], best)

    def each(first, last, body):
        def step(i, carry):
            body(i)
            return carry
        lax.fori_loop(first, last, step, 0)

    half = slots // 2

    def arrived(which, first, last):
        for k in range(first, last):
            which(k).wait_recv()

    for i in range(CUT):
        for k in range(1, EARLY + 1):
            exchange_some(k, i).wait_recv()
            to_prev_some(k, i).start()
            to_next_some(k, i).start()
    for k in range(1, EARLY + 1):
        to_partner(k).start()
    for k in range(EARLY + 1, groups):
        exchange(k).wait_recv()
        to_prev(k).start()
        to_next(k).start()
        to_partner(k).start()
        if k == 6:
            for i in range(1, groups):
                meta(i).wait_recv()
            for t in range(tiles):
                first = meta_send[0] if t == 0 else meta_recv[2 * t]
                rank_lane[OWN, t : t + 1, :] = jnp.where(left, first, meta_recv[2 * t + 1])[0:1]
            for c in rank_copies:
                c.start()
            spread(OWN)
        if k == 7:
            score(OWN, 0, part, OWN, 0, part)
        if k == 8:
            score(OWN, 0, 2 * part, OWN, part, part)
        if k == 9:
            for c in rank_copies:
                c.wait_recv()
            spread(PARTNER)
        if k == 10:
            arrived(to_prev, 0, 4)
            score(OWN, 0, half, NEXT, 0, part)
        if k == 11:
            arrived(to_partner, 0, 8)
            score(PARTNER, 0, half, NEXT, 0, part)
        if k == 12:
            spread(PREV)
        if k == 13:
            score(OWN, 0, 3 * part, OWN, 2 * part, part)
        if k == 14:
            arrived(to_next, 0, 4)
            score(PREV, 0, part, NEXT, 0, part)

    score(OWN, half, half, NEXT, 0, part)
    score(OWN, 0, slots, OWN, 3 * part, part)
    arrived(to_partner, 8, groups)
    score(PARTNER, half, half, NEXT, 0, part)
    each(0, 2, lambda i: score(core, 0, slots, 1 - core, pl.multiple_of(core * half + i * part, part), part))

    last = slots // part - 1
    for j in range(1, last):
        now = j * part
        arrived(to_prev, 4 * j, 4 * j + 4)
        score(OWN, 0, slots, NEXT, now, part)
        score(PARTNER, 0, slots, NEXT, now, part)
        arrived(to_next, 4 * j, 4 * j + 4)
        score(PREV, now, part, NEXT, 0, now)
        score(PREV, 0, now + part, NEXT, now, part)

    def gather(which, t):
        tile = jnp.transpose(sub_acc[which, t * 128 : (t + 1) * 128, :])
        return jnp.max(tile, axis=0, keepdims=True)

    def along(which, t):
        return jnp.max(lane_acc[which, t], axis=0, keepdims=True)

    homes = {PREV: prev_seen, PARTNER: partner, NEXT: next_same, OWN: {}}

    def back(which, k):
        return copy(
            result.at[which, k // 2], returned.at[which, k], back_s.at[which], back_r.at[which],
            {**behind(k), **homes[which]},
        )

    def send_back(which):
        for k in range(1 if which == OWN else 0, groups):
            back(which, k).start()

    now = last * part
    arrived(to_next, 4 * last, groups)
    arrived(to_prev, 4 * last, groups)
    score(PREV, now, part, NEXT, 0, now)
    score(PREV, 0, now + part, NEXT, now, part)
    for t in range(tiles):
        result[PREV, t] = gather(PREV, t)
    score(PARTNER, 0, slots, NEXT, now, part)
    send_back(PREV)
    for t in range(tiles):
        result[PARTNER, t] = jnp.maximum(gather(PARTNER, t), along(PARTNER, t))
    score(OWN, 0, slots, NEXT, now, part)
    for t in range(tiles):
        result[NEXT, t] = along(NEXT, t)
    send_back(NEXT)
    send_back(PARTNER)
    for t in range(tiles):
        result[OWN, t] = jnp.maximum(gather(OWN, t), along(OWN, t))
    send_back(OWN)

    def all_back(which):
        first = 1 if which == OWN else 0
        return copy(
            returned.at[which, first:groups], returned.at[which, first:groups],
            back_s.at[which], back_r.at[which], partner,
        )

    for which in (OWN, PARTNER, NEXT, PREV):
        all_back(which).wait_recv()
    found = []
    for t in range(tiles):
        pair = []
        for k in (2 * t, 2 * t + 1):
            one = result[OWN, 0] if k == 0 else returned[OWN, k]
            for which in (PARTNER, NEXT, PREV):
                one = jnp.maximum(one, returned[which, k])
            pair.append(one)
        found.append(jnp.where(left[0:1], pair[0], pair[1]))
    got = jnp.concatenate(found, axis=1)
    one = got.astype(jnp.bfloat16).astype(jnp.float32)
    rest = got - one
    two = rest.astype(jnp.bfloat16).astype(jnp.float32)
    line8 = lax.broadcasted_iota(jnp.int32, (8, slots), 0)
    terms = jnp.where(
        line8 == 0, one, jnp.where(line8 == 1, two, jnp.where(line8 == 2, rest - two, 0.0))
    ).astype(jnp.bfloat16)
    out = jnp.dot(terms, onehot[...], preferred_element_type=jnp.float32)
    out_ref[...] = jnp.sum(out, axis=0, keepdims=True)

    copy(send.at[slot:slots], buf.at[OWN, slot:slots], own_s.at[OWN], own_r.at[OWN, 1], partner).wait_send()
    for which in (PARTNER, NEXT, PREV):
        copy(buf.at[OWN], buf.at[which], own_s.at[which], own_r.at[which, 0], partner).wait_send()
    copy(meta_send.at[1:groups], meta_recv.at[1:groups], meta_s, meta_r.at[1], partner).wait_send()
    for c in rank_copies:
        c.wait_send()
    for which in (OWN, PARTNER, NEXT, PREV):
        all_back(which).wait_send()


def local(embeddings, cluster_ids, rank_key):
    rows, depth = embeddings.shape
    groups, members = lax.axis_size("grp"), lax.axis_size("blk")
    slot = 2 * rows // groups
    slots = groups * slot
    dma = pltpu.SemaphoreType.DMA
    out = pl.pallas_call(
        functools.partial(kernel, groups=groups, members=members, slot=slot),
        out_shape=jax.ShapeDtypeStruct((1, rows), jnp.float32),
        in_specs=[pl.BlockSpec(memory_space=pltpu.HBM)] * 3,
        out_specs=pl.BlockSpec(memory_space=pltpu.VMEM),
        scratch_shapes=[
            pltpu.VMEM((rows, depth), jnp.bfloat16),
            pltpu.VMEM((1, rows), jnp.int32),
            pltpu.VMEM((1, rows), jnp.int32),
            pltpu.VMEM((4, slots, depth), jnp.bfloat16),
            pltpu.VMEM((slots, depth), jnp.bfloat16),
            pltpu.VMEM((slots, rows), jnp.bfloat16),
            pltpu.VMEM((groups, 8, 128), jnp.float32),
            pltpu.VMEM((groups, 8, 128), jnp.float32),
            pltpu.VMEM((4, slots // 128, 128), jnp.float32),
            pltpu.VMEM((4, slots, 128), jnp.float32),
            pltpu.VMEM((4, slots // 128, 8, 128), jnp.float32),
            pltpu.VMEM((4, slots, 128), jnp.float32),
            pltpu.VMEM((4, slots // 128, 1, 128), jnp.float32),
            pltpu.VMEM((4, groups, 1, 128), jnp.float32),
            dma((3,)),
            dma, dma((groups,)),
            dma((4,)), dma((4, groups)),
            dma((4,)), dma((4,)),
            dma((4,)), dma((4,)), dma((EARLY + 1, CUT)),
        ],
        compiler_params=pltpu.CompilerParams(
            collective_id=0, has_side_effects=True, vmem_limit_bytes=48 * 1024 * 1024
        ),
    )(embeddings, cluster_ids.reshape(1, rows), rank_key.reshape(1, rows))
    return out.reshape(rows)


def solution(mesh):
    placed = (P(("grp", "blk"), None), P(("grp", "blk")), P(("grp", "blk")))
    return jax.shard_map(
        local, mesh=mesh, in_specs=placed, out_specs=P(("grp", "blk")), check_vma=False
    )
```

```python
import functools

import jax
import jax.numpy as jnp
from jax import lax
from jax.experimental import pallas as pl
from jax.experimental.pallas import tpu as pltpu
from jax.sharding import PartitionSpec as P

MESH = pl.DeviceIdType.MESH
epsilon = 1e-06
FAR = 1.0e6
OWN, PARTNER, NEXT, PREV = range(4)
SPLIT = 512
EARLY, CUT = 2, 2


STEPS = (
    (0, 0), (0, 1), (0, 3), (1, 0), (3, 0), (1, 1), (3, 3), (1, 3),
    (3, 1), (0, 2), (2, 0), (1, 2), (2, 1), (3, 2), (2, 3), (2, 2),
)


def kernel(
    emb_hbm, cl_hbm, rk_hbm, out_ref,
    emb, cl, rk, buf, send, onehot, meta_send, meta_recv, rank_lane, rank_sub, lane_acc, sub_acc,
    result, returned,
    in_s, meta_s, meta_r, own_s, own_r, rank_s, rank_r, back_s, back_r, early_r,
    *, groups, members, slot,
):
    rows, depth = emb.shape
    slots = groups * slot
    tiles = slots // 128
    chips = members // 2
    group, member = lax.axis_index("grp"), lax.axis_index("blk")
    chip, core = member // 2, lax.rem(member, 2)
    after, before = lax.rem(chip + 1, chips), lax.rem(chip + chips - 1, chips)
    partner = {"blk": chip * 2 + 1 - core}
    next_same, next_other = {"blk": after * 2 + core}, {"blk": after * 2 + 1 - core}
    crossed = after // (chips // 2)
    next_seen = {"blk": after * 2 + lax.rem(core + crossed, 2)}
    prev_seen = {"blk": before * 2 + lax.rem(core + chip // (chips // 2), 2)}
    prev_same, prev_other = {"blk": before * 2 + core}, {"blk": before * 2 + 1 - core}
    gz, gx = group // 4, lax.rem(group, 4)

    fetch = [
        pltpu.make_async_copy(cl_hbm, cl, in_s.at[0]),
        pltpu.make_async_copy(emb_hbm, emb, in_s.at[1]),
        pltpu.make_async_copy(rk_hbm, rk, in_s.at[2]),
    ]
    for c in fetch:
        c.start()

    def group_at(k, sign):
        dz, dx = STEPS[k]
        dz, dx = (sign * dz) % 4, (sign * dx) % 4
        return lax.rem(gz + dz, 4) * 4 + lax.rem(gx + dx, 4)

    def ahead(k):
        return {"grp": group_at(k, 1)}

    def behind(k):
        return {"grp": group_at(k, -1)}

    barrier = pltpu.get_barrier_semaphore()
    for k in range(1, groups):
        pl.semaphore_signal(barrier, inc=1, device_id=ahead(k), device_id_type=MESH)
    for peer in (partner, next_same, next_other, prev_same, prev_other):
        pl.semaphore_signal(barrier, inc=1, device_id=peer, device_id_type=MESH)

    def copy(src, dst, ssem, rsem, peer):
        return pltpu.make_async_remote_copy(
            src_ref=src, dst_ref=dst, send_sem=ssem, recv_sem=rsem,
            device_id=peer, device_id_type=MESH,
        )

    def piece(k):
        return pl.ds(k * slot, slot)

    def exchange(k):
        return copy(send.at[piece(k)], buf.at[OWN, piece(k)], own_s.at[OWN], own_r.at[OWN, k], ahead(k))

    def some(k, i):
        return pl.ds(k * slot + i * (slot // CUT), slot // CUT)

    def exchange_some(k, i):
        return copy(send.at[some(k, i)], buf.at[OWN, some(k, i)], own_s.at[OWN], early_r.at[k, i], ahead(k))

    def to_prev_some(k, i):
        return copy(buf.at[OWN, some(k, i)], buf.at[NEXT, some(k, i)], own_s.at[NEXT], own_r.at[NEXT, k], prev_same)

    def to_next_some(k, i):
        return copy(buf.at[OWN, some(k, i)], buf.at[PREV, some(k, i)], own_s.at[PREV], own_r.at[PREV, k], next_seen)

    def to_partner(k):
        return copy(buf.at[OWN, piece(k)], buf.at[PARTNER, piece(k)], own_s.at[PARTNER], own_r.at[PARTNER, k], partner)

    def to_prev(k):
        return copy(buf.at[OWN, piece(k)], buf.at[NEXT, piece(k)], own_s.at[NEXT], own_r.at[NEXT, k], prev_same)

    def to_next(k):
        return copy(buf.at[OWN, piece(k)], buf.at[PREV, piece(k)], own_s.at[PREV], own_r.at[PREV, k], next_seen)

    def meta(k):
        return copy(meta_send.at[k], meta_recv.at[k], meta_s, meta_r.at[k], ahead(k))

    lines = lax.broadcasted_iota(jnp.int32, (groups, rows), 0)
    owner = jnp.full((groups, rows), group, jnp.int32)
    for k in range(1, groups):
        owner = jnp.where(lines == k, group_at(k, 1), owner)
    earlier = lax.broadcasted_iota(jnp.int32, (rows, rows), 0) < lax.broadcasted_iota(jnp.int32, (rows, rows), 1)
    earlier = jnp.where(earlier, 1.0, 0.0).astype(jnp.bfloat16)
    fetch[0].wait()
    fetch[1].wait()
    mine = lax.bitwise_and(cl[...], groups - 1) == owner
    count = jnp.dot(
        jnp.where(mine, 1.0, 0.0).astype(jnp.bfloat16), earlier, preferred_element_type=jnp.float32
    )
    target = jnp.sum(
        jnp.where(mine, count + (lines * slot).astype(jnp.float32), 0.0), axis=0, keepdims=True
    )
    part = 4 * slot

    def place(j):
        at = (lax.broadcasted_iota(jnp.int32, (part, rows), 0) + j * part).astype(jnp.float32)
        onehot[j * part : (j + 1) * part, :] = jnp.where(at == target, 1.0, 0.0).astype(jnp.bfloat16)

    def pack(j):
        return jnp.dot(
            onehot[j * part : (j + 1) * part, :], unit, preferred_element_type=jnp.float32
        ).astype(jnp.bfloat16)

    place(0)
    values = emb[...].astype(jnp.float32)
    squares = jnp.sum(values * values, axis=1, keepdims=True)
    unit = (values * lax.rsqrt(squares + epsilon)).astype(jnp.bfloat16)
    packed = pack(0)
    buf[OWN, 0:slot, :] = packed[0:slot]
    send[0:part, :] = packed
    pl.semaphore_wait(barrier, groups - 1 + 5)
    for i in range(CUT):
        for k in range(1, EARLY + 1):
            exchange_some(k, i).start()
        if i == 0:
            to_prev(0).start()
            to_next(0).start()
    for k in range(EARLY + 1, 4):
        exchange(k).start()
    to_partner(0).start()

    def give(j):
        send[j * part : (j + 1) * part, :] = pack(j)
        for k in range(4 * j, 4 * j + 4):
            exchange(k).start()

    place(1)
    give(1)
    for j in range(2, slots // part):
        place(j)
    fetch[2].wait()
    rank = rk[...]
    line8 = lax.broadcasted_iota(jnp.int32, (8, rows), 0)
    high = lax.shift_right_logical(rank, 8).astype(jnp.float32)
    low = lax.bitwise_and(rank, 255).astype(jnp.float32)
    table = jnp.where(line8 == 0, high, jnp.where(line8 == 1, low, 1.0)).astype(jnp.bfloat16)
    found = lax.dot_general(
        table, onehot[...], (((1,), (1,)), ((), ())), preferred_element_type=jnp.float32
    )
    spot = found[0:1] * 256.0 + found[1:2] + (1.0 - found[2:3]) * FAR
    left = lax.broadcasted_iota(jnp.int32, (8, 128), 1) < slot
    for t in range(tiles):
        tile = jnp.broadcast_to(spot[:, t * 128 : (t + 1) * 128], (8, 128))
        turned = pltpu.roll(tile, slot, 1)
        meta_send[2 * t] = jnp.where(left, tile, turned)
        meta_send[2 * t + 1] = jnp.where(left, turned, tile)
    for k in range(1, groups):
        meta(k).start()
    for j in range(2, slots // part):
        give(j)

    lane_acc[...] = jnp.full(lane_acc.shape, -1.0, jnp.float32)
    sub_acc[...] = jnp.full(sub_acc.shape, -1.0, jnp.float32)

    rank_copies = [
        copy(rank_lane.at[OWN], rank_lane.at[PARTNER], rank_s.at[PARTNER], rank_r.at[PARTNER], partner),
        copy(rank_lane.at[OWN], rank_lane.at[NEXT], rank_s.at[NEXT], rank_r.at[NEXT], prev_same),
        copy(rank_lane.at[OWN], rank_lane.at[PREV], rank_s.at[PREV], rank_r.at[PREV], next_seen),
    ]

    def spread(which):
        for t in range(tiles):
            tile = jnp.broadcast_to(rank_lane[which, t : t + 1, :], (128, 128))
            rank_sub[which, t * 128 : (t + 1) * 128, :] = jnp.transpose(tile)

    def score(x, x0, size, y, y0, width, same=False):
        top = [jnp.full((8, 128), -1.0, jnp.float32)] * (width // 128)
        for m in range(0, size, SPLIT):
            cut = min(SPLIT, size - m)
            at = pl.ds(x0 + m, cut)
            here = rank_sub[x, at, :]
            best = sub_acc[x, at, :]
            s = lax.dot_general(
                buf[x, at, :], buf[y, pl.ds(y0, width), :], (((1,), (1,)), ((), ())),
                preferred_element_type=jnp.float32,
            )
            for h in range(width // 128):
                sh = s[:, h * 128 : (h + 1) * 128]
                there = rank_lane[y, pl.ds(y0 // 128 + h, 1), :]
                down = there < here
                best = jnp.maximum(best, jnp.where(down, sh, -1.0))
                up = jnp.where(here < there, sh, -1.0) if same else jnp.where(down, -1.0, sh)
                top[h] = jnp.maximum(top[h], jnp.max(up.reshape(cut // 8, 8, 128), axis=0))
            sub_acc[x, at, :] = best
        for h in range(width // 128):
            t = y0 // 128 + h
            lane_acc[y, t] = jnp.maximum(lane_acc[y, t], top[h])

    def each(first, last, body):
        def step(i, carry):
            body(i)
            return carry
        lax.fori_loop(first, last, step, 0)

    half = slots // 2

    def arrived(which, first, last):
        for k in range(first, last):
            which(k).wait_recv()

    for i in range(CUT):
        for k in range(1, EARLY + 1):
            exchange_some(k, i).wait_recv()
            to_prev_some(k, i).start()
            to_next_some(k, i).start()
    for k in range(1, EARLY + 1):
        to_partner(k).start()
    for k in range(EARLY + 1, groups):
        exchange(k).wait_recv()
        to_prev(k).start()
        to_next(k).start()
        to_partner(k).start()
        if k == 6:
            for i in range(1, groups):
                meta(i).wait_recv()
            for t in range(tiles):
                first = meta_send[0] if t == 0 else meta_recv[2 * t]
                rank_lane[OWN, t : t + 1, :] = jnp.where(left, first, meta_recv[2 * t + 1])[0:1]
            for c in rank_copies:
                c.start()
            spread(OWN)
        if k == 7:
            score(OWN, 0, part, OWN, 0, part, True)
        if k == 8:
            score(OWN, 0, 2 * part, OWN, part, part, True)
        if k == 9:
            for c in rank_copies:
                c.wait_recv()
            spread(PARTNER)
        if k == 10:
            arrived(to_prev, 0, 4)
            score(OWN, 0, half, NEXT, 0, part)
        if k == 11:
            arrived(to_partner, 0, 8)
            score(PARTNER, 0, half, NEXT, 0, part)
        if k == 12:
            spread(PREV)
        if k == 13:
            score(OWN, 0, 3 * part, OWN, 2 * part, part, True)
        if k == 14:
            arrived(to_next, 0, 4)
            score(PREV, 0, part, NEXT, 0, part)

    score(OWN, half, half, NEXT, 0, part)
    score(OWN, 0, slots, OWN, 3 * part, part, True)
    arrived(to_partner, 8, groups)
    score(PARTNER, half, half, NEXT, 0, part)
    each(0, 2, lambda i: score(core, 0, slots, 1 - core, pl.multiple_of(core * half + i * part, part), part))

    last = slots // part - 1
    for j in range(1, last):
        now = j * part
        arrived(to_prev, 4 * j, 4 * j + 4)
        score(OWN, 0, slots, NEXT, now, part)
        score(PARTNER, 0, slots, NEXT, now, part)
        arrived(to_next, 4 * j, 4 * j + 4)
        score(PREV, now, part, NEXT, 0, now)
        score(PREV, 0, now + part, NEXT, now, part)

    def gather(which, t):
        tile = jnp.transpose(sub_acc[which, t * 128 : (t + 1) * 128, :])
        return jnp.max(tile, axis=0, keepdims=True)

    def along(which, t):
        return jnp.max(lane_acc[which, t], axis=0, keepdims=True)

    homes = {PREV: prev_seen, PARTNER: partner, NEXT: next_same, OWN: {}}

    def back(which, k):
        return copy(
            result.at[which, k // 2], returned.at[which, k], back_s.at[which], back_r.at[which],
            {**behind(k), **homes[which]},
        )

    def send_back(which):
        for k in reversed(range(1 if which == OWN else 0, groups)):
            back(which, k).start()

    now = last * part
    arrived(to_next, 4 * last, groups)
    arrived(to_prev, 4 * last, groups)
    score(PREV, now, part, NEXT, 0, now)
    score(PREV, 0, now + part, NEXT, now, part)
    for t in range(tiles):
        result[PREV, t] = gather(PREV, t)
    score(PARTNER, 0, slots, NEXT, now, part)
    send_back(PREV)
    for t in range(tiles):
        result[PARTNER, t] = jnp.maximum(gather(PARTNER, t), along(PARTNER, t))
    score(OWN, 0, slots, NEXT, now, part)
    for t in range(tiles):
        result[NEXT, t] = along(NEXT, t)
    send_back(NEXT)
    send_back(PARTNER)
    for t in range(tiles):
        result[OWN, t] = jnp.maximum(gather(OWN, t), along(OWN, t))
    send_back(OWN)

    def all_back(which):
        first = 1 if which == OWN else 0
        return copy(
            returned.at[which, first:groups], returned.at[which, first:groups],
            back_s.at[which], back_r.at[which], partner,
        )

    for which in (OWN, PARTNER, NEXT, PREV):
        all_back(which).wait_recv()
    found = []
    for t in range(tiles):
        pair = []
        for k in (2 * t, 2 * t + 1):
            one = result[OWN, 0] if k == 0 else returned[OWN, k]
            for which in (PARTNER, NEXT, PREV):
                one = jnp.maximum(one, returned[which, k])
            pair.append(one)
        found.append(jnp.where(left[0:1], pair[0], pair[1]))
    got = jnp.concatenate(found, axis=1)
    one = got.astype(jnp.bfloat16).astype(jnp.float32)
    rest = got - one
    two = rest.astype(jnp.bfloat16).astype(jnp.float32)
    line8 = lax.broadcasted_iota(jnp.int32, (8, slots), 0)
    terms = jnp.where(
        line8 == 0, one, jnp.where(line8 == 1, two, jnp.where(line8 == 2, rest - two, 0.0))
    ).astype(jnp.bfloat16)
    out = jnp.dot(terms, onehot[...], preferred_element_type=jnp.float32)
    out_ref[...] = jnp.sum(out, axis=0, keepdims=True)

    copy(send.at[slot:slots], buf.at[OWN, slot:slots], own_s.at[OWN], own_r.at[OWN, 1], partner).wait_send()
    for which in (PARTNER, NEXT, PREV):
        copy(buf.at[OWN], buf.at[which], own_s.at[which], own_r.at[which, 0], partner).wait_send()
    copy(meta_send.at[1:groups], meta_recv.at[1:groups], meta_s, meta_r.at[1], partner).wait_send()
    for c in rank_copies:
        c.wait_send()
    for which in (OWN, PARTNER, NEXT, PREV):
        all_back(which).wait_send()


def local(embeddings, cluster_ids, rank_key):
    rows, depth = embeddings.shape
    groups, members = lax.axis_size("grp"), lax.axis_size("blk")
    slot = 2 * rows // groups
    slots = groups * slot
    dma = pltpu.SemaphoreType.DMA
    out = pl.pallas_call(
        functools.partial(kernel, groups=groups, members=members, slot=slot),
        out_shape=jax.ShapeDtypeStruct((1, rows), jnp.float32),
        in_specs=[pl.BlockSpec(memory_space=pltpu.HBM)] * 3,
        out_specs=pl.BlockSpec(memory_space=pltpu.VMEM),
        scratch_shapes=[
            pltpu.VMEM((rows, depth), jnp.bfloat16),
            pltpu.VMEM((1, rows), jnp.int32),
            pltpu.VMEM((1, rows), jnp.int32),
            pltpu.VMEM((4, slots, depth), jnp.bfloat16),
            pltpu.VMEM((slots, depth), jnp.bfloat16),
            pltpu.VMEM((slots, rows), jnp.bfloat16),
            pltpu.VMEM((groups, 8, 128), jnp.float32),
            pltpu.VMEM((groups, 8, 128), jnp.float32),
            pltpu.VMEM((4, slots // 128, 128), jnp.float32),
            pltpu.VMEM((4, slots, 128), jnp.float32),
            pltpu.VMEM((4, slots // 128, 8, 128), jnp.float32),
            pltpu.VMEM((4, slots, 128), jnp.float32),
            pltpu.VMEM((4, slots // 128, 1, 128), jnp.float32),
            pltpu.VMEM((4, groups, 1, 128), jnp.float32),
            dma((3,)),
            dma, dma((groups,)),
            dma((4,)), dma((4, groups)),
            dma((4,)), dma((4,)),
            dma((4,)), dma((4,)), dma((EARLY + 1, CUT)),
        ],
        compiler_params=pltpu.CompilerParams(
            collective_id=0, has_side_effects=True, vmem_limit_bytes=48 * 1024 * 1024
        ),
    )(embeddings, cluster_ids.reshape(1, rows), rank_key.reshape(1, rows))
    return out.reshape(rows)


def solution(mesh):
    placed = (P(("grp", "blk"), None), P(("grp", "blk")), P(("grp", "blk")))
    return jax.shard_map(
        local, mesh=mesh, in_specs=placed, out_specs=P(("grp", "blk")), check_vma=False
    )
```

```python
import functools

import jax
import jax.numpy as jnp
from jax import lax
from jax.experimental import pallas as pl
from jax.experimental.pallas import tpu as pltpu
from jax.sharding import PartitionSpec as P

MESH = pl.DeviceIdType.MESH
epsilon = 1e-06
FAR = 1.0e6
OWN, PARTNER, NEXT, PREV = range(4)
SPLIT = 512
EARLY, CUT = 2, 2


STEPS = (
    (0, 0), (0, 1), (0, 3), (1, 0), (3, 0), (1, 1), (3, 3), (1, 3),
    (3, 1), (0, 2), (2, 0), (1, 2), (2, 1), (3, 2), (2, 3), (2, 2),
)


def kernel(
    emb_hbm, cl_hbm, rk_hbm, out_ref,
    emb, cl, rk, buf, send, onehot, meta_send, meta_recv, rank_lane, rank_sub, lane_acc, sub_acc,
    result, returned,
    in_s, meta_s, meta_r, own_s, own_r, rank_s, rank_r, back_s, back_r, early_r, wider,
    *, groups, members, slot,
):
    rows, depth = emb.shape
    slots = groups * slot
    tiles = slots // 128
    chips = members // 2
    group, member = lax.axis_index("grp"), lax.axis_index("blk")
    chip, core = member // 2, lax.rem(member, 2)
    after, before = lax.rem(chip + 1, chips), lax.rem(chip + chips - 1, chips)
    partner = {"blk": chip * 2 + 1 - core}
    next_same, next_other = {"blk": after * 2 + core}, {"blk": after * 2 + 1 - core}
    crossed = after // (chips // 2)
    next_seen = {"blk": after * 2 + lax.rem(core + crossed, 2)}
    prev_seen = {"blk": before * 2 + lax.rem(core + chip // (chips // 2), 2)}
    prev_same, prev_other = {"blk": before * 2 + core}, {"blk": before * 2 + 1 - core}
    gz, gx = group // 4, lax.rem(group, 4)

    fetch = [
        pltpu.make_async_copy(cl_hbm, cl, in_s.at[0]),
        pltpu.make_async_copy(emb_hbm, emb, in_s.at[1]),
        pltpu.make_async_copy(rk_hbm, rk, in_s.at[2]),
    ]
    for c in fetch:
        c.start()

    def group_at(k, sign):
        dz, dx = STEPS[k]
        dz, dx = (sign * dz) % 4, (sign * dx) % 4
        return lax.rem(gz + dz, 4) * 4 + lax.rem(gx + dx, 4)

    def ahead(k):
        return {"grp": group_at(k, 1)}

    def behind(k):
        return {"grp": group_at(k, -1)}

    barrier = pltpu.get_barrier_semaphore()
    sides = [ahead(k) for k in range(1, 5)]
    for peer in sides + [partner, next_same, next_other, prev_same, prev_other]:
        pl.semaphore_signal(barrier, inc=1, device_id=peer, device_id_type=MESH)

    def widen(i):
        for peer in sides:
            pl.semaphore_signal(wider.at[i], inc=1, device_id=peer, device_id_type=MESH)

    def copy(src, dst, ssem, rsem, peer):
        return pltpu.make_async_remote_copy(
            src_ref=src, dst_ref=dst, send_sem=ssem, recv_sem=rsem,
            device_id=peer, device_id_type=MESH,
        )

    def piece(k):
        return pl.ds(k * slot, slot)

    def exchange(k):
        return copy(send.at[piece(k)], buf.at[OWN, piece(k)], own_s.at[OWN], own_r.at[OWN, k], ahead(k))

    def some(k, i):
        return pl.ds(k * slot + i * (slot // CUT), slot // CUT)

    def exchange_some(k, i):
        return copy(send.at[some(k, i)], buf.at[OWN, some(k, i)], own_s.at[OWN], early_r.at[k, i], ahead(k))

    def to_prev_some(k, i):
        return copy(buf.at[OWN, some(k, i)], buf.at[NEXT, some(k, i)], own_s.at[NEXT], own_r.at[NEXT, k], prev_same)

    def to_next_some(k, i):
        return copy(buf.at[OWN, some(k, i)], buf.at[PREV, some(k, i)], own_s.at[PREV], own_r.at[PREV, k], next_seen)

    def to_partner(k):
        return copy(buf.at[OWN, piece(k)], buf.at[PARTNER, piece(k)], own_s.at[PARTNER], own_r.at[PARTNER, k], partner)

    def to_prev(k):
        return copy(buf.at[OWN, piece(k)], buf.at[NEXT, piece(k)], own_s.at[NEXT], own_r.at[NEXT, k], prev_same)

    def to_next(k):
        return copy(buf.at[OWN, piece(k)], buf.at[PREV, piece(k)], own_s.at[PREV], own_r.at[PREV, k], next_seen)

    def meta(k):
        return copy(meta_send.at[k], meta_recv.at[k], meta_s, meta_r.at[k], ahead(k))

    lines = lax.broadcasted_iota(jnp.int32, (groups, rows), 0)
    owner = jnp.full((groups, rows), group, jnp.int32)
    for k in range(1, groups):
        owner = jnp.where(lines == k, group_at(k, 1), owner)
    earlier = lax.broadcasted_iota(jnp.int32, (rows, rows), 0) < lax.broadcasted_iota(jnp.int32, (rows, rows), 1)
    earlier = jnp.where(earlier, 1.0, 0.0).astype(jnp.bfloat16)
    fetch[0].wait()
    fetch[1].wait()
    mine = lax.bitwise_and(cl[...], groups - 1) == owner
    count = jnp.dot(
        jnp.where(mine, 1.0, 0.0).astype(jnp.bfloat16), earlier, preferred_element_type=jnp.float32
    )
    target = jnp.sum(
        jnp.where(mine, count + (lines * slot).astype(jnp.float32), 0.0), axis=0, keepdims=True
    )
    part = 4 * slot

    def place(j):
        at = (lax.broadcasted_iota(jnp.int32, (part, rows), 0) + j * part).astype(jnp.float32)
        onehot[j * part : (j + 1) * part, :] = jnp.where(at == target, 1.0, 0.0).astype(jnp.bfloat16)

    def pack(j):
        return jnp.dot(
            onehot[j * part : (j + 1) * part, :], unit, preferred_element_type=jnp.float32
        ).astype(jnp.bfloat16)

    place(0)
    values = emb[...].astype(jnp.float32)
    squares = jnp.sum(values * values, axis=1, keepdims=True)
    unit = (values * lax.rsqrt(squares + epsilon)).astype(jnp.bfloat16)
    packed = pack(0)
    buf[OWN, 0:slot, :] = packed[0:slot]
    send[0:part, :] = packed
    pl.semaphore_wait(barrier, 9)
    widen(0)
    for i in range(CUT):
        for k in range(1, EARLY + 1):
            exchange_some(k, i).start()
        if i == 0:
            to_prev(0).start()
            to_next(0).start()
    for k in range(EARLY + 1, 4):
        exchange(k).start()
    to_partner(0).start()

    def give(j):
        send[j * part : (j + 1) * part, :] = pack(j)

    place(1)
    give(1)
    exchange(4).start()
    pl.semaphore_wait(wider.at[0], 4)
    widen(1)
    for j in range(2, slots // part):
        place(j)
    fetch[2].wait()
    rank = rk[...]
    line8 = lax.broadcasted_iota(jnp.int32, (8, rows), 0)
    high = lax.shift_right_logical(rank, 8).astype(jnp.float32)
    low = lax.bitwise_and(rank, 255).astype(jnp.float32)
    table = jnp.where(line8 == 0, high, jnp.where(line8 == 1, low, 1.0)).astype(jnp.bfloat16)
    found = lax.dot_general(
        table, onehot[...], (((1,), (1,)), ((), ())), preferred_element_type=jnp.float32
    )
    spot = found[0:1] * 256.0 + found[1:2] + (1.0 - found[2:3]) * FAR
    left = lax.broadcasted_iota(jnp.int32, (8, 128), 1) < slot
    for t in range(tiles):
        tile = jnp.broadcast_to(spot[:, t * 128 : (t + 1) * 128], (8, 128))
        turned = pltpu.roll(tile, slot, 1)
        meta_send[2 * t] = jnp.where(left, tile, turned)
        meta_send[2 * t + 1] = jnp.where(left, turned, tile)
    pl.semaphore_wait(wider.at[1], 4)
    widen(2)
    for k in range(5, 8):
        exchange(k).start()
    for i in range(CUT):
        for k in range(1, EARLY + 1):
            exchange_some(k, i).wait_recv()
            to_prev_some(k, i).start()
            to_next_some(k, i).start()
    for k in range(1, EARLY + 1):
        to_partner(k).start()
    give(2)
    pl.semaphore_wait(wider.at[2], 4)
    for k in range(1, groups):
        meta(k).start()
    for k in range(8, 12):
        exchange(k).start()
    give(3)
    for k in range(12, groups):
        exchange(k).start()

    lane_acc[...] = jnp.full(lane_acc.shape, -1.0, jnp.float32)
    sub_acc[...] = jnp.full(sub_acc.shape, -1.0, jnp.float32)

    rank_copies = [
        copy(rank_lane.at[OWN], rank_lane.at[PARTNER], rank_s.at[PARTNER], rank_r.at[PARTNER], partner),
        copy(rank_lane.at[OWN], rank_lane.at[NEXT], rank_s.at[NEXT], rank_r.at[NEXT], prev_same),
        copy(rank_lane.at[OWN], rank_lane.at[PREV], rank_s.at[PREV], rank_r.at[PREV], next_seen),
    ]

    def spread(which):
        for t in range(tiles):
            tile = jnp.broadcast_to(rank_lane[which, t : t + 1, :], (128, 128))
            rank_sub[which, t * 128 : (t + 1) * 128, :] = jnp.transpose(tile)

    def score(x, x0, size, y, y0, width, same=False):
        top = [jnp.full((8, 128), -1.0, jnp.float32)] * (width // 128)
        for m in range(0, size, SPLIT):
            cut = min(SPLIT, size - m)
            at = pl.ds(x0 + m, cut)
            here = rank_sub[x, at, :]
            best = sub_acc[x, at, :]
            s = lax.dot_general(
                buf[x, at, :], buf[y, pl.ds(y0, width), :], (((1,), (1,)), ((), ())),
                preferred_element_type=jnp.float32,
            )
            for h in range(width // 128):
                sh = s[:, h * 128 : (h + 1) * 128]
                there = rank_lane[y, pl.ds(y0 // 128 + h, 1), :]
                down = there < here
                best = jnp.maximum(best, jnp.where(down, sh, -1.0))
                up = jnp.where(here < there, sh, -1.0) if same else jnp.where(down, -1.0, sh)
                top[h] = jnp.maximum(top[h], jnp.max(up.reshape(cut // 8, 8, 128), axis=0))
            sub_acc[x, at, :] = best
        for h in range(width // 128):
            t = y0 // 128 + h
            lane_acc[y, t] = jnp.maximum(lane_acc[y, t], top[h])

    def each(first, last, body):
        def step(i, carry):
            body(i)
            return carry
        lax.fori_loop(first, last, step, 0)

    half = slots // 2

    def arrived(which, first, last):
        for k in range(first, last):
            which(k).wait_recv()

    for k in range(EARLY + 1, groups):
        exchange(k).wait_recv()
        to_prev(k).start()
        to_next(k).start()
        to_partner(k).start()
        if k == 7:
            for i in range(1, groups):
                meta(i).wait_recv()
            for t in range(tiles):
                first = meta_send[0] if t == 0 else meta_recv[2 * t]
                rank_lane[OWN, t : t + 1, :] = jnp.where(left, first, meta_recv[2 * t + 1])[0:1]
            for c in rank_copies:
                c.start()
            spread(OWN)
        if k == 8:
            score(OWN, 0, part, OWN, 0, part, True)
        if k == 9:
            score(OWN, 0, 2 * part, OWN, part, part, True)
        if k == 11:
            for c in rank_copies:
                c.wait_recv()
            spread(PARTNER)
        if k == 12:
            arrived(to_prev, 0, 4)
            score(OWN, 0, half, NEXT, 0, part)
        if k == 13:
            arrived(to_partner, 0, 8)
            score(PARTNER, 0, half, NEXT, 0, part)
        if k == 14:
            spread(PREV)
        if k == 12:
            score(OWN, 0, 3 * part, OWN, 2 * part, part, True)

    arrived(to_next, 0, 4)
    score(PREV, 0, part, NEXT, 0, part)
    score(OWN, half, half, NEXT, 0, part)
    score(OWN, 0, slots, OWN, 3 * part, part, True)
    arrived(to_partner, 8, groups)
    score(PARTNER, half, half, NEXT, 0, part)
    each(0, 2, lambda i: score(core, 0, slots, 1 - core, pl.multiple_of(core * half + i * part, part), part))

    last = slots // part - 1
    for j in range(1, last):
        now = j * part
        arrived(to_prev, 4 * j, 4 * j + 4)
        score(OWN, 0, slots, NEXT, now, part)
        score(PARTNER, 0, slots, NEXT, now, part)
        arrived(to_next, 4 * j, 4 * j + 4)
        score(PREV, now, part, NEXT, 0, now)
        score(PREV, 0, now + part, NEXT, now, part)

    def gather(which, t):
        tile = jnp.transpose(sub_acc[which, t * 128 : (t + 1) * 128, :])
        return jnp.max(tile, axis=0, keepdims=True)

    def along(which, t):
        return jnp.max(lane_acc[which, t], axis=0, keepdims=True)

    homes = {PREV: prev_seen, PARTNER: partner, NEXT: next_same, OWN: {}}

    def back(which, k):
        return copy(
            result.at[which, k // 2], returned.at[which, k], back_s.at[which], back_r.at[which],
            {**behind(k), **homes[which]},
        )

    def send_back(which):
        for k in reversed(range(1 if which == OWN else 0, groups)):
            back(which, k).start()

    now = last * part
    arrived(to_next, 4 * last, groups)
    arrived(to_prev, 4 * last, groups)
    score(PREV, now, part, NEXT, 0, now)
    score(PREV, 0, now + part, NEXT, now, part)
    for t in range(tiles):
        result[PREV, t] = gather(PREV, t)
    score(PARTNER, 0, slots, NEXT, now, part)
    send_back(PREV)
    for t in range(tiles):
        result[PARTNER, t] = jnp.maximum(gather(PARTNER, t), along(PARTNER, t))
    score(OWN, 0, slots, NEXT, now, part)
    for t in range(tiles):
        result[NEXT, t] = along(NEXT, t)
    send_back(NEXT)
    send_back(PARTNER)
    for t in range(tiles):
        result[OWN, t] = jnp.maximum(gather(OWN, t), along(OWN, t))
    send_back(OWN)

    def all_back(which):
        first = 1 if which == OWN else 0
        return copy(
            returned.at[which, first:groups], returned.at[which, first:groups],
            back_s.at[which], back_r.at[which], partner,
        )

    for which in (OWN, PARTNER, NEXT, PREV):
        all_back(which).wait_recv()
    found = []
    for t in range(tiles):
        pair = []
        for k in (2 * t, 2 * t + 1):
            one = result[OWN, 0] if k == 0 else returned[OWN, k]
            for which in (PARTNER, NEXT, PREV):
                one = jnp.maximum(one, returned[which, k])
            pair.append(one)
        found.append(jnp.where(left[0:1], pair[0], pair[1]))
    got = jnp.concatenate(found, axis=1)
    one = got.astype(jnp.bfloat16).astype(jnp.float32)
    rest = got - one
    two = rest.astype(jnp.bfloat16).astype(jnp.float32)
    line8 = lax.broadcasted_iota(jnp.int32, (8, slots), 0)
    terms = jnp.where(
        line8 == 0, one, jnp.where(line8 == 1, two, jnp.where(line8 == 2, rest - two, 0.0))
    ).astype(jnp.bfloat16)
    out = jnp.dot(terms, onehot[...], preferred_element_type=jnp.float32)
    out_ref[...] = jnp.sum(out, axis=0, keepdims=True)

    copy(send.at[slot:slots], buf.at[OWN, slot:slots], own_s.at[OWN], own_r.at[OWN, 1], partner).wait_send()
    for which in (PARTNER, NEXT, PREV):
        copy(buf.at[OWN], buf.at[which], own_s.at[which], own_r.at[which, 0], partner).wait_send()
    copy(meta_send.at[1:groups], meta_recv.at[1:groups], meta_s, meta_r.at[1], partner).wait_send()
    for c in rank_copies:
        c.wait_send()
    for which in (OWN, PARTNER, NEXT, PREV):
        all_back(which).wait_send()


def local(embeddings, cluster_ids, rank_key):
    rows, depth = embeddings.shape
    groups, members = lax.axis_size("grp"), lax.axis_size("blk")
    slot = 2 * rows // groups
    slots = groups * slot
    dma = pltpu.SemaphoreType.DMA
    out = pl.pallas_call(
        functools.partial(kernel, groups=groups, members=members, slot=slot),
        out_shape=jax.ShapeDtypeStruct((1, rows), jnp.float32),
        in_specs=[pl.BlockSpec(memory_space=pltpu.HBM)] * 3,
        out_specs=pl.BlockSpec(memory_space=pltpu.VMEM),
        scratch_shapes=[
            pltpu.VMEM((rows, depth), jnp.bfloat16),
            pltpu.VMEM((1, rows), jnp.int32),
            pltpu.VMEM((1, rows), jnp.int32),
            pltpu.VMEM((4, slots, depth), jnp.bfloat16),
            pltpu.VMEM((slots, depth), jnp.bfloat16),
            pltpu.VMEM((slots, rows), jnp.bfloat16),
            pltpu.VMEM((groups, 8, 128), jnp.float32),
            pltpu.VMEM((groups, 8, 128), jnp.float32),
            pltpu.VMEM((4, slots // 128, 128), jnp.float32),
            pltpu.VMEM((4, slots, 128), jnp.float32),
            pltpu.VMEM((4, slots // 128, 8, 128), jnp.float32),
            pltpu.VMEM((4, slots, 128), jnp.float32),
            pltpu.VMEM((4, slots // 128, 1, 128), jnp.float32),
            pltpu.VMEM((4, groups, 1, 128), jnp.float32),
            dma((3,)),
            dma, dma((groups,)),
            dma((4,)), dma((4, groups)),
            dma((4,)), dma((4,)),
            dma((4,)), dma((4,)), dma((EARLY + 1, CUT)),
            pltpu.SemaphoreType.REGULAR((3,)),
        ],
        compiler_params=pltpu.CompilerParams(
            collective_id=0, has_side_effects=True, vmem_limit_bytes=48 * 1024 * 1024
        ),
    )(embeddings, cluster_ids.reshape(1, rows), rank_key.reshape(1, rows))
    return out.reshape(rows)


def solution(mesh):
    placed = (P(("grp", "blk"), None), P(("grp", "blk")), P(("grp", "blk")))
    return jax.shard_map(
        local, mesh=mesh, in_specs=placed, out_specs=P(("grp", "blk")), check_vma=False
    )
```

```python
import functools

import jax
import jax.numpy as jnp
from jax import lax
from jax.experimental import pallas as pl
from jax.experimental.pallas import tpu as pltpu
from jax.sharding import PartitionSpec as P

MESH = pl.DeviceIdType.MESH
epsilon = 1e-06
FAR = 1.0e6
OWN, PARTNER, NEXT, PREV = range(4)
SPLIT = 512
EARLY, CUT = 2, 2


STEPS = (
    (0, 0), (0, 1), (0, 3), (1, 0), (3, 0), (1, 1), (3, 3), (1, 3),
    (3, 1), (0, 2), (2, 0), (1, 2), (2, 1), (3, 2), (2, 3), (2, 2),
)


def kernel(
    emb_hbm, cl_hbm, rk_hbm, out_ref,
    emb, cl, rk, buf, send, onehot, meta_send, meta_recv, rank_lane, rank_sub, lane_acc, sub_acc,
    result, returned,
    in_s, meta_s, meta_r, own_s, own_r, rank_s, rank_r, back_s, back_r, early_r,
    *, groups, members, slot,
):
    rows, depth = emb.shape
    slots = groups * slot
    tiles = slots // 128
    chips = members // 2
    group, member = lax.axis_index("grp"), lax.axis_index("blk")
    chip, core = member // 2, lax.rem(member, 2)
    after, before = lax.rem(chip + 1, chips), lax.rem(chip + chips - 1, chips)
    partner = {"blk": chip * 2 + 1 - core}
    next_same, next_other = {"blk": after * 2 + core}, {"blk": after * 2 + 1 - core}
    crossed = after // (chips // 2)
    next_seen = {"blk": after * 2 + lax.rem(core + crossed, 2)}
    prev_seen = {"blk": before * 2 + lax.rem(core + chip // (chips // 2), 2)}
    prev_same, prev_other = {"blk": before * 2 + core}, {"blk": before * 2 + 1 - core}
    gz, gx = group // 4, lax.rem(group, 4)

    fetch = [
        pltpu.make_async_copy(cl_hbm, cl, in_s.at[0]),
        pltpu.make_async_copy(emb_hbm, emb, in_s.at[1]),
        pltpu.make_async_copy(rk_hbm, rk, in_s.at[2]),
    ]
    for c in fetch:
        c.start()

    def group_at(k, sign):
        dz, dx = STEPS[k]
        dz, dx = (sign * dz) % 4, (sign * dx) % 4
        return lax.rem(gz + dz, 4) * 4 + lax.rem(gx + dx, 4)

    def ahead(k):
        return {"grp": group_at(k, 1)}

    def behind(k):
        return {"grp": group_at(k, -1)}

    barrier = pltpu.get_barrier_semaphore()
    for k in range(1, groups):
        pl.semaphore_signal(barrier, inc=1, device_id=ahead(k), device_id_type=MESH)
    for peer in (partner, next_same, next_other, prev_same, prev_other):
        pl.semaphore_signal(barrier, inc=1, device_id=peer, device_id_type=MESH)

    def copy(src, dst, ssem, rsem, peer):
        return pltpu.make_async_remote_copy(
            src_ref=src, dst_ref=dst, send_sem=ssem, recv_sem=rsem,
            device_id=peer, device_id_type=MESH,
        )

    def piece(k):
        return pl.ds(k * slot, slot)

    def exchange(k):
        return copy(send.at[piece(k)], buf.at[OWN, piece(k)], own_s.at[OWN], own_r.at[OWN, k], ahead(k))

    def some(k, i):
        return pl.ds(k * slot + i * (slot // CUT), slot // CUT)

    def exchange_some(k, i):
        return copy(send.at[some(k, i)], buf.at[OWN, some(k, i)], own_s.at[OWN], early_r.at[k, i], ahead(k))

    def to_prev_some(k, i):
        return copy(buf.at[OWN, some(k, i)], buf.at[NEXT, some(k, i)], own_s.at[NEXT], own_r.at[NEXT, k], prev_same)

    def to_next_some(k, i):
        return copy(buf.at[OWN, some(k, i)], buf.at[PREV, some(k, i)], own_s.at[PREV], own_r.at[PREV, k], next_seen)

    def to_partner(k):
        return copy(buf.at[OWN, piece(k)], buf.at[PARTNER, piece(k)], own_s.at[PARTNER], own_r.at[PARTNER, k], partner)

    def to_prev(k):
        return copy(buf.at[OWN, piece(k)], buf.at[NEXT, piece(k)], own_s.at[NEXT], own_r.at[NEXT, k], prev_same)

    def to_next(k):
        return copy(buf.at[OWN, piece(k)], buf.at[PREV, piece(k)], own_s.at[PREV], own_r.at[PREV, k], next_seen)

    def meta(k):
        return copy(meta_send.at[k], meta_recv.at[k], meta_s, meta_r.at[k], ahead(k))

    lines = lax.broadcasted_iota(jnp.int32, (groups, rows), 0)
    owner = jnp.full((groups, rows), group, jnp.int32)
    for k in range(1, groups):
        owner = jnp.where(lines == k, group_at(k, 1), owner)
    earlier = lax.broadcasted_iota(jnp.int32, (rows, rows), 0) < lax.broadcasted_iota(jnp.int32, (rows, rows), 1)
    earlier = jnp.where(earlier, 1.0, 0.0).astype(jnp.bfloat16)
    fetch[0].wait()
    fetch[1].wait()
    mine = lax.bitwise_and(cl[...], groups - 1) == owner
    count = jnp.dot(
        jnp.where(mine, 1.0, 0.0).astype(jnp.bfloat16), earlier, preferred_element_type=jnp.float32
    )
    target = jnp.sum(
        jnp.where(mine, count + (lines * slot).astype(jnp.float32), 0.0), axis=0, keepdims=True
    )
    part = 4 * slot

    def place(j):
        at = (lax.broadcasted_iota(jnp.int32, (part, rows), 0) + j * part).astype(jnp.float32)
        onehot[j * part : (j + 1) * part, :] = jnp.where(at == target, 1.0, 0.0).astype(jnp.bfloat16)

    def pack(j):
        return jnp.dot(
            onehot[j * part : (j + 1) * part, :], unit, preferred_element_type=jnp.float32
        ).astype(jnp.bfloat16)

    place(0)
    values = emb[...].astype(jnp.float32)
    squares = jnp.sum(values * values, axis=1, keepdims=True)
    unit = (values * lax.rsqrt(squares + epsilon)).astype(jnp.bfloat16)
    packed = pack(0)
    buf[OWN, 0:slot, :] = packed[0:slot]
    send[0:part, :] = packed
    pl.semaphore_wait(barrier, groups - 1 + 5)
    for i in range(CUT):
        for k in range(1, EARLY + 1):
            exchange_some(k, i).start()
        if i == 0:
            to_prev(0).start()
            to_next(0).start()
    for k in range(EARLY + 1, 4):
        exchange(k).start()
    to_partner(0).start()

    def give(j):
        send[j * part : (j + 1) * part, :] = pack(j)
        for k in range(4 * j, 4 * j + 4):
            exchange(k).start()

    place(1)
    give(1)
    for j in range(2, slots // part):
        place(j)
    fetch[2].wait()
    rank = rk[...]
    line8 = lax.broadcasted_iota(jnp.int32, (8, rows), 0)
    high = lax.shift_right_logical(rank, 8).astype(jnp.float32)
    low = lax.bitwise_and(rank, 255).astype(jnp.float32)
    table = jnp.where(line8 == 0, high, jnp.where(line8 == 1, low, 1.0)).astype(jnp.bfloat16)
    found = lax.dot_general(
        table, onehot[...], (((1,), (1,)), ((), ())), preferred_element_type=jnp.float32
    )
    spot = found[0:1] * 256.0 + found[1:2] + (1.0 - found[2:3]) * FAR
    left = lax.broadcasted_iota(jnp.int32, (8, 128), 1) < slot
    for t in range(tiles):
        tile = jnp.broadcast_to(spot[:, t * 128 : (t + 1) * 128], (8, 128))
        turned = pltpu.roll(tile, slot, 1)
        meta_send[2 * t] = jnp.where(left, tile, turned)
        meta_send[2 * t + 1] = jnp.where(left, turned, tile)
    for k in range(1, groups):
        meta(k).start()
    for j in range(2, slots // part):
        give(j)

    lane_acc[...] = jnp.full(lane_acc.shape, -1.0, jnp.float32)
    sub_acc[...] = jnp.full(sub_acc.shape, -1.0, jnp.float32)

    rank_copies = [
        copy(rank_lane.at[OWN], rank_lane.at[PARTNER], rank_s.at[PARTNER], rank_r.at[PARTNER], partner),
        copy(rank_lane.at[OWN], rank_lane.at[NEXT], rank_s.at[NEXT], rank_r.at[NEXT], prev_same),
        copy(rank_lane.at[OWN], rank_lane.at[PREV], rank_s.at[PREV], rank_r.at[PREV], next_seen),
    ]

    def spread(which):
        for t in range(tiles):
            tile = jnp.broadcast_to(rank_lane[which, t : t + 1, :], (128, 128))
            rank_sub[which, t * 128 : (t + 1) * 128, :] = jnp.transpose(tile)

    def score(x, x0, size, y, y0, width, same=False):
        top = [jnp.full((8, 128), -1.0, jnp.float32)] * (width // 128)
        for m in range(0, size, SPLIT):
            cut = min(SPLIT, size - m)
            at = pl.ds(x0 + m, cut)
            here = rank_sub[x, at, :]
            best = sub_acc[x, at, :]
            s = lax.dot_general(
                buf[x, at, :], buf[y, pl.ds(y0, width), :], (((1,), (1,)), ((), ())),
                preferred_element_type=jnp.float32,
            )
            for h in range(width // 128):
                sh = s[:, h * 128 : (h + 1) * 128]
                there = rank_lane[y, pl.ds(y0 // 128 + h, 1), :]
                down = there < here
                best = jnp.maximum(best, jnp.where(down, sh, -1.0))
                up = jnp.where(here < there, sh, -1.0) if same else jnp.where(down, -1.0, sh)
                top[h] = jnp.maximum(top[h], jnp.max(up.reshape(cut // 8, 8, 128), axis=0))
            sub_acc[x, at, :] = best
        for h in range(width // 128):
            t = y0 // 128 + h
            lane_acc[y, t] = jnp.maximum(lane_acc[y, t], top[h])

    def each(first, last, body):
        def step(i, carry):
            body(i)
            return carry
        lax.fori_loop(first, last, step, 0)

    half = slots // 2

    def arrived(which, first, last):
        for k in range(first, last):
            which(k).wait_recv()

    for i in range(CUT):
        for k in range(1, EARLY + 1):
            exchange_some(k, i).wait_recv()
            to_prev_some(k, i).start()
            to_next_some(k, i).start()
    for k in range(1, EARLY + 1):
        to_partner(k).start()
    for k in range(EARLY + 1, groups):
        exchange(k).wait_recv()
        to_prev(k).start()
        to_next(k).start()
        to_partner(k).start()
        if k == 6:
            for i in range(1, groups):
                meta(i).wait_recv()
            for t in range(tiles):
                first = meta_send[0] if t == 0 else meta_recv[2 * t]
                rank_lane[OWN, t : t + 1, :] = jnp.where(left, first, meta_recv[2 * t + 1])[0:1]
            for c in rank_copies:
                c.start()
            spread(OWN)
        if k == 7:
            score(OWN, 0, part, OWN, 0, part, True)
        if k == 8:
            score(OWN, 0, 2 * part, OWN, part, part, True)
        if k == 9:
            for c in rank_copies:
                c.wait_recv()
            spread(PARTNER)
        if k == 10:
            arrived(to_prev, 0, 4)
            score(OWN, 0, half, NEXT, 0, part)
        if k == 11:
            arrived(to_partner, 0, 8)
            score(PARTNER, 0, half, NEXT, 0, part)
        if k == 12:
            spread(PREV)
        if k == 13:
            score(OWN, 0, 3 * part, OWN, 2 * part, part, True)
        if k == 14:
            arrived(to_next, 0, 4)
            score(PREV, 0, part, NEXT, 0, part)

    score(OWN, half, half, NEXT, 0, part)
    score(OWN, 0, slots, OWN, 3 * part, part, True)
    arrived(to_partner, 8, groups)
    score(PARTNER, half, half, NEXT, 0, part)
    each(0, 2, lambda i: score(core, 0, slots, 1 - core, pl.multiple_of(core * half + i * part, part), part))

    last = slots // part - 1
    for j in range(1, last):
        now = j * part
        arrived(to_prev, 4 * j, 4 * j + 4)
        score(OWN, 0, slots, NEXT, now, part)
        score(PARTNER, 0, slots, NEXT, now, part)
        arrived(to_next, 4 * j, 4 * j + 4)
        score(PREV, now, part, NEXT, 0, now)
        score(PREV, 0, now + part, NEXT, now, part)

    def gather(which, t):
        tile = jnp.transpose(sub_acc[which, t * 128 : (t + 1) * 128, :])
        return jnp.max(tile, axis=0, keepdims=True)

    def along(which, t):
        return jnp.max(lane_acc[which, t], axis=0, keepdims=True)

    homes = {PREV: prev_seen, PARTNER: partner, NEXT: next_same, OWN: {}}

    def back(which, k):
        return copy(
            result.at[which, k // 2], returned.at[which, k], back_s.at[which], back_r.at[which],
            {**behind(k), **homes[which]},
        )

    def send_back(which):
        for k in reversed(range(1 if which == OWN else 0, groups)):
            back(which, k).start()

    now = last * part
    arrived(to_next, 4 * last, groups)
    arrived(to_prev, 4 * last, groups)
    score(PREV, now, part, NEXT, 0, now)
    score(PREV, 0, now + part, NEXT, now, part)
    for t in range(tiles):
        result[PREV, t] = gather(PREV, t)
    score(PARTNER, 0, slots, NEXT, now, part)
    send_back(PREV)
    for t in range(tiles):
        result[PARTNER, t] = jnp.maximum(gather(PARTNER, t), along(PARTNER, t))
    score(OWN, 0, half, NEXT, now, part)
    for t in range(tiles // 2):
        result[OWN, t] = jnp.maximum(gather(OWN, t), along(OWN, t))
    score(OWN, half, half, NEXT, now, part)
    for t in range(tiles):
        result[NEXT, t] = along(NEXT, t)
    send_back(NEXT)
    send_back(PARTNER)
    for t in range(tiles // 2, tiles):
        result[OWN, t] = jnp.maximum(gather(OWN, t), along(OWN, t))
    send_back(OWN)

    def all_back(which):
        first = 1 if which == OWN else 0
        return copy(
            returned.at[which, first:groups], returned.at[which, first:groups],
            back_s.at[which], back_r.at[which], partner,
        )

    for which in (OWN, PARTNER, NEXT, PREV):
        all_back(which).wait_recv()
    found = []
    for t in range(tiles):
        pair = []
        for k in (2 * t, 2 * t + 1):
            one = result[OWN, 0] if k == 0 else returned[OWN, k]
            for which in (PARTNER, NEXT, PREV):
                one = jnp.maximum(one, returned[which, k])
            pair.append(one)
        found.append(jnp.where(left[0:1], pair[0], pair[1]))
    got = jnp.concatenate(found, axis=1)
    one = got.astype(jnp.bfloat16).astype(jnp.float32)
    rest = got - one
    two = rest.astype(jnp.bfloat16).astype(jnp.float32)
    line8 = lax.broadcasted_iota(jnp.int32, (8, slots), 0)
    terms = jnp.where(
        line8 == 0, one, jnp.where(line8 == 1, two, jnp.where(line8 == 2, rest - two, 0.0))
    ).astype(jnp.bfloat16)
    out = jnp.dot(terms, onehot[...], preferred_element_type=jnp.float32)
    out_ref[...] = jnp.sum(out, axis=0, keepdims=True)

    copy(send.at[slot:slots], buf.at[OWN, slot:slots], own_s.at[OWN], own_r.at[OWN, 1], partner).wait_send()
    for which in (PARTNER, NEXT, PREV):
        copy(buf.at[OWN], buf.at[which], own_s.at[which], own_r.at[which, 0], partner).wait_send()
    copy(meta_send.at[1:groups], meta_recv.at[1:groups], meta_s, meta_r.at[1], partner).wait_send()
    for c in rank_copies:
        c.wait_send()
    for which in (OWN, PARTNER, NEXT, PREV):
        all_back(which).wait_send()


def local(embeddings, cluster_ids, rank_key):
    rows, depth = embeddings.shape
    groups, members = lax.axis_size("grp"), lax.axis_size("blk")
    slot = 2 * rows // groups
    slots = groups * slot
    dma = pltpu.SemaphoreType.DMA
    out = pl.pallas_call(
        functools.partial(kernel, groups=groups, members=members, slot=slot),
        out_shape=jax.ShapeDtypeStruct((1, rows), jnp.float32),
        in_specs=[pl.BlockSpec(memory_space=pltpu.HBM)] * 3,
        out_specs=pl.BlockSpec(memory_space=pltpu.VMEM),
        scratch_shapes=[
            pltpu.VMEM((rows, depth), jnp.bfloat16),
            pltpu.VMEM((1, rows), jnp.int32),
            pltpu.VMEM((1, rows), jnp.int32),
            pltpu.VMEM((4, slots, depth), jnp.bfloat16),
            pltpu.VMEM((slots, depth), jnp.bfloat16),
            pltpu.VMEM((slots, rows), jnp.bfloat16),
            pltpu.VMEM((groups, 8, 128), jnp.float32),
            pltpu.VMEM((groups, 8, 128), jnp.float32),
            pltpu.VMEM((4, slots // 128, 128), jnp.float32),
            pltpu.VMEM((4, slots, 128), jnp.float32),
            pltpu.VMEM((4, slots // 128, 8, 128), jnp.float32),
            pltpu.VMEM((4, slots, 128), jnp.float32),
            pltpu.VMEM((4, slots // 128, 1, 128), jnp.float32),
            pltpu.VMEM((4, groups, 1, 128), jnp.float32),
            dma((3,)),
            dma, dma((groups,)),
            dma((4,)), dma((4, groups)),
            dma((4,)), dma((4,)),
            dma((4,)), dma((4,)), dma((EARLY + 1, CUT)),
        ],
        compiler_params=pltpu.CompilerParams(
            collective_id=0, has_side_effects=True, vmem_limit_bytes=48 * 1024 * 1024
        ),
    )(embeddings, cluster_ids.reshape(1, rows), rank_key.reshape(1, rows))
    return out.reshape(rows)


def solution(mesh):
    placed = (P(("grp", "blk"), None), P(("grp", "blk")), P(("grp", "blk")))
    return jax.shard_map(
        local, mesh=mesh, in_specs=placed, out_specs=P(("grp", "blk")), check_vma=False
    )
```
